32 devices in a mesh: dom: 8 (over y, x, core), col: 4 (over z).
Axes of the slice: x: 2, y: 2, z: 4, core: 2. Of those that a mesh axis runs over, the one named last changes fastest.
Arguments:
- features: bfloat16 [65536, 1024], P('dom', 'col'), may hold values from -6 to 6
- requests: int32 [8, 8, 8], P('dom'), may hold values from 0 to 63
- counts: int32 [8, 8], P(None, 'dom'), may hold values from 0 to 8, as said below
- tile_block: int32 [128, 32], P('dom'), may hold values from 0 to 31
- local_nbr: int32 [16384, 128], P('dom'), may hold values from 0 to 127
- tile_count: int32 [128], P('dom'), may hold values from 1 to 32, as said below
- w_self: bfloat16 [1024, 1024], P('col'), may hold values from -0.125 to 0.125
- w_neigh: bfloat16 [1024, 1024], P('col'), may hold values from -0.75 to 0.75
Outputs:
- embeddings: bfloat16 [16384, 1024], P('dom', 'col')
The draws below stay inside these ranges and needn't reach their ends.
Inputs may be any that keep to these rules, and one draw needn't show every extreme that they name: Each shard's counts over all partitions sum to 32; for every shard some partition has exactly 8. `tile_count`: on every shard some destination block uses all 32 tiles.
All inputs are finite; a program needn't handle non-finite values.
Results may differ from the reference program's by a relative error of at most 0.014.
Values may be sent and summed in bfloat16 or wider, within the bound.
A program may use at most 128 MiB of HBM per device.

```python
import jax
import jax.numpy as jnp
from jax import lax

D = 1024
BLOCK_ROWS = 128
BLK_DEV = 64
CAP = 8
DST_BLK = 16
TILES = 32
FAN_T = 4
FRONT = 32
BLOCKS = 512
DST_BLOCKS = 128
COL_W = 256
N_DOM = 8


def draw_counts(key, part):
    key_order, key_share, key_heat = jax.random.split(key, 3)
    heat = jax.random.permutation(key_heat, N_DOM)
    orders = jax.vmap(lambda subkey: jax.random.permutation(subkey, N_DOM))(jax.random.split(key_order, N_DOM))
    share = jax.random.randint(key_share, (N_DOM, N_DOM // 2), 0, CAP + 1)
    share = share.at[:, 0].set(CAP)
    first_half = orders[:, 0::2]
    second_half = orders[:, 1::2]
    larger = jnp.maximum(share, CAP - share)
    hotter = heat[first_half] > heat[second_half]
    first_count = jnp.where(hotter, larger, CAP - larger)
    second_count = CAP - first_count
    shard_rows = jnp.arange(N_DOM)[:, None]
    grid = jnp.zeros((N_DOM, N_DOM), jnp.int32)
    grid = grid.at[shard_rows, first_half].set(first_count)
    grid = grid.at[shard_rows, second_half].set(second_count)
    return grid.T.astype(jnp.int32)


def draw_tile_count(key, part):
    key_level, key_raw, key_where = jax.random.split(key, 3)
    levels = jax.random.randint(key_level, (N_DOM, 1), TILES // 4, TILES + 1)
    raw_bits = jax.random.randint(key_raw, (N_DOM, DST_BLK), 0, 1 << 20)
    result = 1 + raw_bits % levels
    full_at = jax.random.randint(key_where, (N_DOM, 1), 0, DST_BLK)
    result = jnp.where(jnp.arange(DST_BLK)[None, :] == full_at, TILES, result)
    return result.reshape(-1).astype(jnp.int32)


def place_ends(drawn, own_key, low, high):
    index_at = [jax.random.randint(jax.random.fold_in(own_key, axis), (), 0, length) for axis, length in enumerate(drawn.shape)]
    main_axis = drawn.shape.index(max(drawn.shape))
    neighbour = index_at[:main_axis] + [(index_at[main_axis] + 1) % drawn.shape[main_axis]] + index_at[main_axis + 1:]
    return drawn.at[tuple(index_at)].set(low).at[tuple(neighbour)].set(high)


def level_of(rng, dims, cuts, low, top_value):
    loudness, own = 1.0, jax.random.fold_in(rng, 6)
    for position, shards_of in cuts:
        heights = jnp.exp(jax.random.uniform(jax.random.fold_in(own, position), (shards_of,), jnp.float32, low / len(cuts), top_value / len(cuts)))
        loudness = loudness * jnp.repeat(heights, dims[position] // shards_of).reshape([-1 if axis == position else 1 for axis in range(len(dims))])
    return loudness


def gaussian(rng, extent, spread, bound, cuts=(), kind=jnp.bfloat16):
    entries = jax.random.normal(rng, extent, jnp.float32) * spread
    if len(cuts) > 0:
        entries = level_of(rng, extent, cuts, -0.22, 0.18) * entries
    return jnp.clip(entries, min=-bound, max=bound).astype(kind)


def setup_inputs(seed: int = 0) -> dict:
    seeds = jax.random.split(jax.random.key(seed), 9)
    return {
        "features": gaussian(seeds[0], (BLOCKS * BLOCK_ROWS, D), 1.0, 6.0, ((0, 8), (1, 4))),
        "requests": place_ends(jax.random.randint(seeds[1], (N_DOM, N_DOM, CAP), 0, BLK_DEV), jax.random.fold_in(seeds[1], 1), 0, BLK_DEV - 1).astype(jnp.int32),
        "counts": draw_counts(jax.random.fold_in(seeds[8], 71), 0),
        "tile_block": place_ends(jax.random.randint(seeds[3], (DST_BLOCKS, TILES), 0, FRONT), jax.random.fold_in(seeds[3], 1), 0, FRONT - 1).astype(jnp.int32),
        "local_nbr": place_ends(jax.random.randint(seeds[4], (DST_BLOCKS * BLOCK_ROWS, TILES * FAN_T), 0, BLOCK_ROWS), jax.random.fold_in(seeds[4], 1), 0, BLOCK_ROWS - 1).astype(jnp.int32),
        "tile_count": draw_tile_count(jax.random.fold_in(seeds[8], 71), 0),
        "w_self": gaussian(seeds[6], (D, D), (2 * D) ** -0.5, 0.125, ((0, 4),)),
        "w_neigh": gaussian(seeds[7], (D, D), (D // 16) ** -0.5, 0.75, ((0, 4),)),
    }


def frontier_blocks(requests, counts):
    slot_ends = jnp.cumsum(counts, axis=0)
    slot_starts = slot_ends - counts
    positions = jnp.arange(FRONT, dtype=jnp.int32)

    def one_shard(ends_col, starts_col, wanted):
        owner_of = lax.optimization_barrier(jnp.sum((ends_col[None, :] <= positions[:, None]).astype(jnp.int32), axis=1))
        slot_pos = positions - starts_col[owner_of]
        return (owner_of * BLK_DEV + wanted[owner_of, slot_pos]).astype(jnp.int32)
    return jax.vmap(one_shard, in_axes=(1, 1, 1))(slot_ends, slot_starts, requests)

def reference(features, requests, counts, tile_block, local_nbr, tile_count, w_self, w_neigh):
    global_block = frontier_blocks(requests, counts)
    tile_ids = jnp.arange(TILES, dtype=jnp.int32)
    row_ids = jnp.arange(BLOCK_ROWS, dtype=jnp.int32)
    groups = D // COL_W
    self_mat = w_self.astype(jnp.float32).reshape(groups, COL_W, D)
    neigh_mat = w_neigh.astype(jnp.float32).reshape(groups, COL_W, D)

    def one_block(inputs):
        block_id, picks, neighbor, used_tiles = inputs
        shard_row = global_block[block_id // DST_BLK]
        tile_global = shard_row[picks]
        rows = tile_global[None, :, None] * BLOCK_ROWS + neighbor.reshape(BLOCK_ROWS, TILES, FAN_T)
        values = features[rows.reshape(-1)].astype(jnp.float32).reshape(BLOCK_ROWS, TILES, FAN_T, D)
        live_mask = (tile_ids < used_tiles).astype(jnp.float32)
        summed = lax.optimization_barrier(jnp.sum(values * live_mask[None, :, None, None], axis=(1, 2)))
        agg = (summed / (FAN_T * used_tiles).astype(jnp.float32)).astype(jnp.bfloat16)
        own = features[shard_row[block_id % DST_BLK] * BLOCK_ROWS + row_ids]
        pieces = jnp.einsum('rkc,kcj->krj', own.astype(jnp.float32).reshape(BLOCK_ROWS, groups, COL_W), self_mat, precision=lax.Precision.HIGHEST)
        pieces = pieces + jnp.einsum('rkc,kcj->krj', agg.astype(jnp.float32).reshape(BLOCK_ROWS, groups, COL_W), neigh_mat, precision=lax.Precision.HIGHEST)
        pieces = lax.optimization_barrier(pieces.astype(jnp.bfloat16)).astype(jnp.float32)
        hidden = jnp.maximum(lax.optimization_barrier(jnp.sum(pieces, axis=0)), 0.0)
        scale = jnp.sqrt(0.25 + lax.optimization_barrier(jnp.sum(hidden * hidden, axis=1, keepdims=True)) / D)
        return (hidden / scale).astype(jnp.bfloat16)
    block_ids = jnp.arange(DST_BLOCKS, dtype=jnp.int32)
    result = lax.map(one_block, (block_ids, tile_block, local_nbr.reshape(DST_BLOCKS, BLOCK_ROWS, TILES * FAN_T), tile_count))
    return result.reshape(DST_BLOCKS * BLOCK_ROWS, D)
```

```python
import functools

import jax
import jax.numpy as jnp
from jax import lax
from jax.experimental import pallas as pl
from jax.experimental.pallas import tpu as pltpu
from jax.sharding import PartitionSpec as P

D = 1024
BLOCK_ROWS = 128
CAP = 8
TILES = 32
FAN_T = 4
GROUP = 8
PACK = 16


def aggregate_kernel(
    front, width, slot_of, tile_block, tile_count, nbr_ref, arrived, out_ref, held, turned, nbr_t, sems
):
    step = pl.program_id(0)

    def fetch(p):
        return pltpu.make_async_copy(arrived.at[slot_of[p]], held.at[p], sems.at[p])

    @pl.when(step == 0)
    def _():
        def begin(p, carry):
            fetch(p).start()
            return carry

        lax.fori_loop(0, front, begin, 0)

        def finish(i, carry):
            for k in range(4):
                fetch(i * 4 + k).wait()
            for k in range(4):
                turned[i * 4 + k] = held[i * 4 + k].T
            return carry

        lax.fori_loop(0, front // 4, finish, 0)

    nbr_t[...] = nbr_ref[...].astype(jnp.float32).T
    used = tile_count[step]
    shape = (BLOCK_ROWS // PACK, PACK, BLOCK_ROWS)
    row_ids = (
        lax.broadcasted_iota(jnp.int32, shape, 0) * PACK + lax.broadcasted_iota(jnp.int32, shape, 1)
    ).astype(jnp.float32).astype(jnp.bfloat16)
    one = jnp.ones(shape, jnp.bfloat16)
    zero = jnp.zeros(shape, jnp.bfloat16)

    def body(q, acc):
        nbr = nbr_t[pl.ds(pl.multiple_of(q * (GROUP * FAN_T), GROUP * FAN_T), GROUP * FAN_T), :]
        counts = []
        blocks = []
        for i in range(GROUP):
            tile = q * GROUP + i
            total = None
            for f in range(FAN_T):
                row = nbr[i * FAN_T + f : i * FAN_T + f + 1, :]
                row = jnp.where(tile < used, row, -1.0)
                row = jnp.broadcast_to(row, (PACK, BLOCK_ROWS)).astype(jnp.bfloat16)
                hit = jnp.where(row[None] == row_ids, one, zero)
                total = hit if total is None else total + hit
            counts.append(total.reshape(BLOCK_ROWS, BLOCK_ROWS))
            blocks.append(turned[tile_block[step * TILES + tile]])
        lhs = jnp.concatenate(blocks, axis=1)
        rhs = jnp.concatenate(counts, axis=0)
        return acc + jnp.dot(lhs, rhs, preferred_element_type=jnp.float32)

    summed = lax.fori_loop(
        0, (used + GROUP - 1) // GROUP, body, jnp.zeros((width, BLOCK_ROWS), jnp.float32)
    )
    mean = summed / (used * FAN_T).astype(jnp.float32)
    out_ref[:, :width] = held[step]
    out_ref[:, width:] = mean.T.astype(jnp.bfloat16)


def aggregate(arrived, slot_of, tile_block, local_nbr, tile_count):
    front = slot_of.shape[0]
    width = arrived.shape[-1]
    dst_blocks = tile_count.shape[0]
    return pl.pallas_call(
        functools.partial(aggregate_kernel, front, width),
        out_shape=jax.ShapeDtypeStruct((dst_blocks * BLOCK_ROWS, 2 * width), jnp.bfloat16),
        grid_spec=pltpu.PrefetchScalarGridSpec(
            num_scalar_prefetch=3,
            grid=(dst_blocks,),
            in_specs=[
                pl.BlockSpec((BLOCK_ROWS, TILES * FAN_T), lambda i, *_: (i, 0)),
                pl.BlockSpec(memory_space=pl.ANY),
            ],
            out_specs=pl.BlockSpec((BLOCK_ROWS, 2 * width), lambda i, *_: (i, 0)),
            scratch_shapes=[
                pltpu.VMEM((front, BLOCK_ROWS, width), jnp.bfloat16),
                pltpu.VMEM((front, width, BLOCK_ROWS), jnp.bfloat16),
                pltpu.VMEM((TILES * FAN_T, BLOCK_ROWS), jnp.float32),
                pltpu.SemaphoreType.DMA((front,)),
            ],
        ),
        compiler_params=pltpu.CompilerParams(dimension_semantics=("arbitrary",)),
        cost_estimate=pl.CostEstimate(flops=4 * 10**9, bytes_accessed=8 * 2**20, transcendentals=0),
    )(slot_of, tile_block.reshape(-1), tile_count, local_nbr, arrived)


def project_kernel(n_col, width, order, x_ref, *rest):
    w_refs = rest[:-1]
    out_ref = rest[-1]
    total = None
    for s in range(n_col):
        rows = x_ref[order[s]]
        term = jnp.dot(rows[:, :width], w_refs[2 * s][...], preferred_element_type=jnp.float32)
        term = term + jnp.dot(rows[:, width:], w_refs[2 * s + 1][...], preferred_element_type=jnp.float32)
        total = term if total is None else total + term
    hidden = jnp.maximum(total, 0.0)
    squares = jnp.sum(hidden * hidden, axis=1, keepdims=True)
    result = (hidden / jnp.sqrt(0.25 + squares / D)).astype(jnp.bfloat16)
    for k in range(n_col):
        out_ref[k] = result[:, k * width : (k + 1) * width]


def project(mixed, weights, order):
    n_col, rows, _ = mixed.shape
    width = D // n_col
    tile = BLOCK_ROWS
    return pl.pallas_call(
        functools.partial(project_kernel, n_col, width),
        out_shape=jax.ShapeDtypeStruct((n_col, rows, width), jnp.bfloat16),
        grid_spec=pltpu.PrefetchScalarGridSpec(
            num_scalar_prefetch=1,
            grid=(rows // tile,),
            in_specs=[pl.BlockSpec((n_col, tile, 2 * width), lambda i, *_: (0, i, 0))]
            + [pl.BlockSpec((width, D), lambda i, *_: (0, 0)) for _ in weights],
            out_specs=pl.BlockSpec((n_col, tile, width), lambda i, *_: (0, i, 0)),
        ),
        compiler_params=pltpu.CompilerParams(dimension_semantics=("arbitrary",)),
        cost_estimate=pl.CostEstimate(flops=2 * 10**9, bytes_accessed=7 * 2**20, transcendentals=0),
    )(order, mixed, *weights)


MESH = pl.DeviceIdType.MESH
PAIR = 2
NEAR_LAG = 1
SWAP_LAG = 3
SUM_LAG = 5
LINE = 4


def exchange_kernel(n_dom, outgoing, arrived, send, recv, own_sem):
    me = lax.axis_index("dom")

    def copy_to(d):
        peer = lax.rem(me + d, n_dom)
        return pltpu.make_async_remote_copy(
            src_ref=outgoing.at[peer], dst_ref=arrived.at[me], send_sem=send.at[d], recv_sem=recv.at[d],
            device_id={"dom": peer}, device_id_type=MESH,
        )

    own = pltpu.make_async_copy(outgoing.at[me], arrived.at[me], own_sem)
    for d in range(1, n_dom):
        copy_to(d).start()
    own.start()
    own.wait()
    for d in range(1, n_dom):
        copy_to(d).wait_send()
        copy_to(d).wait_recv()


def exchange(outgoing):
    n_dom = outgoing.shape[0]
    anywhere = pl.BlockSpec(memory_space=pl.ANY)
    return pl.pallas_call(
        functools.partial(exchange_kernel, n_dom),
        out_shape=jax.ShapeDtypeStruct(outgoing.shape, outgoing.dtype),
        in_specs=[anywhere],
        out_specs=anywhere,
        scratch_shapes=[
            pltpu.SemaphoreType.DMA((n_dom,)),
            pltpu.SemaphoreType.DMA((n_dom,)),
            pltpu.SemaphoreType.DMA,
        ],
        compiler_params=pltpu.CompilerParams(has_side_effects=True),
    )(outgoing)


def line_kernel(
    n_dom, requests, counts, tile_block, tile_count, features, local_nbr, w_self, w_neigh, out,
    feat, outgoing, arrived, nbr_in, nbr_t, hits, mixed, near, part, part_in, kept, sums, sums_in, passed, passed_in,
    own_w, far_w, turned_w, slot_of,
    load_sem, own_sem, send, recv, w_send, w_recv,
    near_send, near_recv, part_send, part_recv, sum_send, sum_recv, out_send, out_recv,
):
    me = lax.axis_index("dom")
    z = lax.axis_index("col")
    core = lax.rem(me, 2)
    chip = me // 2
    n_chip = n_dom // 2
    front = slot_of.shape[0]
    dst_blocks, span, _ = mixed.shape
    width = span // 2
    at_end = jnp.logical_or(z == 0, z == LINE - 1)
    inside = jnp.logical_not(at_end)
    half = z // 2

    def remote(src, dst, s_sem, r_sem, **device):
        return pltpu.make_async_remote_copy(
            src_ref=src, dst_ref=dst, send_sem=s_sem, recv_sem=r_sem, device_id=device, device_id_type=MESH,
        )

    loads = [
        pltpu.make_async_copy(src, dst, load_sem.at[i])
        for i, (src, dst) in enumerate(
            ((features, feat), (local_nbr, nbr_in), (w_self, own_w.at[0]), (w_neigh, own_w.at[1]))
        )
    ]
    for copy in loads:
        copy.start()

    barrier = pltpu.get_barrier_semaphore()

    def greet(d, carry):
        pl.semaphore_signal(barrier, inc=1, device_id={"dom": lax.rem(me + d, n_dom)}, device_id_type=MESH)
        return carry

    lax.fori_loop(1, n_dom, greet, 0)

    @pl.when(at_end)
    def _():
        pl.semaphore_signal(barrier, inc=1, device_id={"col": 1 + half}, device_id_type=MESH)
        pl.semaphore_wait(barrier, n_dom)

    @pl.when(inside)
    def _():
        pl.semaphore_signal(barrier, inc=1, device_id={"col": 2 - half}, device_id_type=MESH)
        pl.semaphore_signal(barrier, inc=1, device_id={"col": half * (LINE - 1)}, device_id_type=MESH)
        pl.semaphore_wait(barrier, n_dom + 1)

    def weight_copy(i):
        src = w_self if i == 0 else w_neigh
        return remote(src, far_w.at[i], w_send.at[i], w_recv.at[i], col=1 + half)

    @pl.when(at_end)
    def _():
        weight_copy(0).start()
        weight_copy(1).start()

    def slots(owner):
        return pl.ds(owner * CAP, CAP)

    def block_copy(peer, owner):
        return remote(outgoing.at[slots(peer)], arrived.at[slots(owner)], send.at[peer], recv.at[owner], dom=peer)

    def own_copy():
        return pltpu.make_async_copy(outgoing.at[slots(me)], arrived.at[slots(me)], own_sem)

    loads[0].wait()

    def give(j, carry):
        group = j // n_chip
        peer = lax.rem(chip + 1 + lax.rem(j, n_chip), n_chip) * 2 + group
        for s in range(CAP):
            outgoing[peer * CAP + s] = feat[requests[0, peer, s]].T

        @pl.when(peer == me)
        def _():
            own_copy().start()

        @pl.when(peer != me)
        def _():
            block_copy(peer, me).start()

        return carry

    lax.fori_loop(0, n_dom, give, 0)

    ends = []
    end = jnp.int32(0)
    for o in range(n_dom):
        end = end + counts[o]
        ends.append(end)

    def place(p, carry):
        owner = jnp.int32(0)
        start = jnp.int32(0)
        for o in range(n_dom):
            passed_by = ends[o] <= p
            owner = owner + jnp.where(passed_by, 1, 0)
            start = jnp.where(passed_by, ends[o], start)
        slot_of[p] = jnp.minimum(owner * CAP + p - start, n_dom * CAP - 1)
        return carry

    lax.fori_loop(0, front, place, 0)

    loads[1].wait()
    shape = (BLOCK_ROWS // PACK, PACK, BLOCK_ROWS)
    row_ids = (
        lax.broadcasted_iota(jnp.int32, shape, 0) * PACK + lax.broadcasted_iota(jnp.int32, shape, 1)
    ).astype(jnp.float32).astype(jnp.bfloat16)
    one = jnp.ones(shape, jnp.bfloat16)
    zero = jnp.zeros(shape, jnp.bfloat16)
    sample = lax.broadcasted_iota(jnp.int32, (TILES * FAN_T, BLOCK_ROWS), 0)
    groups = TILES // GROUP

    def prepare(b, carry):
        picked = nbr_in[pl.ds(pl.multiple_of(b * BLOCK_ROWS, BLOCK_ROWS), BLOCK_ROWS), :].astype(jnp.float32).T
        nbr_t[...] = jnp.where(sample < tile_count[b] * FAN_T, picked, -1.0)

        def build(q, inner):
            nbr = nbr_t[pl.ds(pl.multiple_of(q * (GROUP * FAN_T), GROUP * FAN_T), GROUP * FAN_T), :]
            for i in range(GROUP):
                total = None
                for f in range(FAN_T):
                    row = nbr[i * FAN_T + f : i * FAN_T + f + 1, :]
                    row = jnp.broadcast_to(row, (PACK, BLOCK_ROWS)).astype(jnp.bfloat16)
                    hit = jnp.where(row[None] == row_ids, one, zero)
                    total = hit if total is None else total + hit
                hits[b * groups + q, i * BLOCK_ROWS : (i + 1) * BLOCK_ROWS, :] = total.reshape(BLOCK_ROWS, BLOCK_ROWS)
            return inner

        return lax.fori_loop(0, groups, build, carry)

    lax.fori_loop(0, dst_blocks, prepare, 0)

    loads[2].wait()
    loads[3].wait()

    @pl.when(inside)
    def _():
        for i in range(2):
            weight_copy(i).wait_recv()
        for h in range(2):
            for i in range(2):
                turned_w[h, :, i * width : (i + 1) * width] = own_w[i, :, h * span : (h + 1) * span].T
                turned_w[h, :, span + i * width : span + (i + 1) * width] = far_w[i, :, h * span : (h + 1) * span].T

    own_copy().wait()

    def take(d, carry):
        owner = lax.rem(me + d, n_dom)
        block_copy(owner, owner).wait_recv()
        return carry

    lax.fori_loop(1, n_dom, take, 0)

    def near_copy(c):
        return remote(mixed.at[c], near.at[c], near_send.at[c], near_recv.at[c], col=1 + half)

    def part_copy(c):
        return remote(part.at[c], part_in.at[c], part_send.at[c], part_recv.at[c], col=2 - half)

    def sum_copy(c):
        return remote(sums.at[c], sums_in.at[c], sum_send.at[c], sum_recv.at[c], col=2 - half)

    def out_copy(c):
        return remote(passed.at[c], passed_in.at[c], out_send.at[c], out_recv.at[c], col=half * (LINE - 1))

    def gather(b):
        used = tile_count[b]
        summed = None
        for q in range(groups):
            blocks = [arrived[slot_of[tile_block[b, q * GROUP + i]]] for i in range(GROUP)]
            term = jnp.dot(
                jnp.concatenate(blocks, axis=1), hits[b * groups + q], preferred_element_type=jnp.float32
            )
            summed = term if summed is None else summed + term
        mean = summed / (used * FAN_T).astype(jnp.float32)
        mixed[b, :width] = arrived[slot_of[b]]
        mixed[b, width:] = mean.astype(jnp.bfloat16)

    def product(c, h):
        own = jnp.concatenate([mixed[c], mixed[c + 1]], axis=1)
        far = jnp.concatenate([near[c], near[c + 1]], axis=1)
        total = jnp.dot(turned_w[h, :, :span], own, preferred_element_type=jnp.float32)
        total = total + jnp.dot(turned_w[h, :, span:], far, preferred_element_type=jnp.float32)
        return total[:, :BLOCK_ROWS], total[:, BLOCK_ROWS:]

    def first(i):
        c = i * PAIR
        for k in range(PAIR):
            near_copy(c + k).wait_recv()
        for k, term in enumerate(product(c, 1 - half)):
            part[c + k] = term.astype(jnp.bfloat16)
            part_copy(c + k).start()
        for k, term in enumerate(product(c, half)):
            kept[c + k] = term

    def second(c):
        part_copy(c).wait_recv()
        hidden = jnp.maximum(kept[c] + part_in[c].astype(jnp.float32), 0.0)
        kept[c] = hidden
        sums[c] = jnp.sum((hidden * hidden).reshape(span // 8, 8, BLOCK_ROWS), axis=0)
        sum_copy(c).start()

    def third(c):
        sum_copy(c).wait_recv()
        squares = jnp.sum(sums[c] + sums_in[c], axis=0, keepdims=True)
        scale = 1.0 / jnp.sqrt(0.25 + squares / D)
        result = (kept[c] * scale).astype(jnp.bfloat16)
        low, high = result[:width], result[width:]
        passed[c] = jnp.where(half == 0, low, high)
        out_copy(c).start()
        rows = pl.ds(pl.multiple_of(c * BLOCK_ROWS, BLOCK_ROWS), BLOCK_ROWS)
        out[rows, :] = jnp.where(half == 0, high, low).T

    @pl.when(at_end)
    def _():
        def send_mixed(c, carry):
            gather(c)
            near_copy(c).start()
            return carry

        lax.fori_loop(0, dst_blocks, send_mixed, 0)

        def receive(c, carry):
            out_copy(c).wait_recv()
            rows = pl.ds(pl.multiple_of(c * BLOCK_ROWS, BLOCK_ROWS), BLOCK_ROWS)
            out[rows, :] = passed_in[c].T
            near_copy(c).wait_send()
            return carry

        lax.fori_loop(0, dst_blocks, receive, 0)
        weight_copy(0).wait_send()
        weight_copy(1).wait_send()

    @pl.when(inside)
    def _():
        def each(work):
            def run(i):
                for k in range(PAIR):
                    work(i * PAIR + k)

            return run

        def stage(i, carry):
            for lag, work in ((0, each(gather)), (NEAR_LAG, first), (SWAP_LAG, each(second)), (SUM_LAG, each(third))):

                @pl.when(jnp.logical_and(i >= lag, i < dst_blocks // PAIR + lag))
                def _(lag=lag, work=work):
                    work(i - lag)

            return carry

        lax.fori_loop(0, dst_blocks // PAIR + SUM_LAG, stage, 0)

        def finish(c, carry):
            part_copy(c).wait_send()
            sum_copy(c).wait_send()
            out_copy(c).wait_send()
            return carry

        lax.fori_loop(0, dst_blocks, finish, 0)

    def sent(d, carry):
        peer = lax.rem(me + d, n_dom)
        block_copy(peer, me).wait_send()
        return carry

    lax.fori_loop(1, n_dom, sent, 0)


def on_line(features, requests, counts, tile_block, local_nbr, tile_count, w_self, w_neigh):
    n_dom = lax.axis_size("dom")
    total, width = local_nbr.shape[0], features.shape[1]
    dst_blocks = total // BLOCK_ROWS
    span = 2 * width
    blocks = features.reshape(-1, BLOCK_ROWS, width)
    anywhere = pl.BlockSpec(memory_space=pl.ANY)
    scalars = pl.BlockSpec(memory_space=pltpu.SMEM)
    dma = pltpu.SemaphoreType.DMA
    bf16, f32 = jnp.bfloat16, jnp.float32
    return pl.pallas_call(
        functools.partial(line_kernel, n_dom),
        out_shape=jax.ShapeDtypeStruct((total, width), bf16),
        in_specs=[scalars] * 4 + [anywhere] * 4,
        out_specs=pl.BlockSpec(memory_space=pltpu.VMEM),
        scratch_shapes=[
            pltpu.VMEM(blocks.shape, bf16),
            pltpu.VMEM((n_dom * CAP, width, BLOCK_ROWS), bf16),
            pltpu.VMEM((n_dom * CAP, width, BLOCK_ROWS), bf16),
            pltpu.VMEM(local_nbr.shape, jnp.int32),
            pltpu.VMEM((TILES * FAN_T, BLOCK_ROWS), f32),
            pltpu.VMEM((dst_blocks * TILES // GROUP, GROUP * BLOCK_ROWS, BLOCK_ROWS), bf16),
            pltpu.VMEM((dst_blocks, span, BLOCK_ROWS), bf16),
            pltpu.VMEM((dst_blocks, span, BLOCK_ROWS), bf16),
            pltpu.VMEM((dst_blocks, span, BLOCK_ROWS), bf16),
            pltpu.VMEM((dst_blocks, span, BLOCK_ROWS), bf16),
            pltpu.VMEM((dst_blocks, span, BLOCK_ROWS), f32),
            pltpu.VMEM((dst_blocks, 8, BLOCK_ROWS), f32),
            pltpu.VMEM((dst_blocks, 8, BLOCK_ROWS), f32),
            pltpu.VMEM((dst_blocks, width, BLOCK_ROWS), bf16),
            pltpu.VMEM((dst_blocks, width, BLOCK_ROWS), bf16),
            pltpu.VMEM((2,) + w_self.shape, bf16),
            pltpu.VMEM((2,) + w_self.shape, bf16),
            pltpu.VMEM((2, span, 2 * span), bf16),
            pltpu.SMEM((n_dom * CAP // 2,), jnp.int32),
            dma((4,)), dma, dma((n_dom,)), dma((n_dom,)), dma((2,)), dma((2,)),
        ]
        + [dma((dst_blocks,))] * 8,
        compiler_params=pltpu.CompilerParams(has_side_effects=True, collective_id=0, vmem_limit_bytes=67_000_000),
    )(requests, counts.reshape(-1), tile_block, tile_count, blocks, local_nbr, w_self, w_neigh)


def on_device(features, requests, counts, tile_block, local_nbr, tile_count, w_self, w_neigh):
    n_dom = lax.axis_size("dom")
    n_col = lax.axis_size("col")
    col_width = features.shape[1]
    if n_col == LINE:
        return on_line(features, requests, counts, tile_block, local_nbr, tile_count, w_self, w_neigh)
    blocks = features.reshape(-1, BLOCK_ROWS, col_width)
    outgoing = blocks.at[requests[0].reshape(-1)].get(mode="promise_in_bounds")
    outgoing = outgoing.reshape(n_dom, CAP, BLOCK_ROWS, col_width)
    arrived = exchange(outgoing).reshape(n_dom * CAP, BLOCK_ROWS, col_width)
    slot_ends = jnp.cumsum(counts[:, 0])
    positions = jnp.arange(n_dom * CAP // 2, dtype=jnp.int32)
    passed = slot_ends[None, :] <= positions[:, None]
    owner_of = jnp.sum(passed.astype(jnp.int32), axis=1)
    start_of = jnp.max(jnp.where(passed, slot_ends[None, :], 0), axis=1)
    slot_of = owner_of * CAP + positions - start_of

    mixed = aggregate(arrived, slot_of, tile_block, local_nbr, tile_count)
    weights = [w_self, w_neigh]
    for shift in range(1, n_col):
        perm = [(k, (k + shift) % n_col) for k in range(n_col)]
        weights.append(lax.ppermute(w_self, "col", perm))
        weights.append(lax.ppermute(w_neigh, "col", perm))
    order = (lax.axis_index("col") - jnp.arange(n_col, dtype=jnp.int32)) % n_col
    mixed = mixed.reshape(n_col, -1, 2 * col_width)
    mixed = lax.all_to_all(mixed, "col", split_axis=0, concat_axis=0, tiled=True)
    result = project(mixed, weights, order)
    result = lax.all_to_all(result, "col", split_axis=0, concat_axis=0, tiled=True)
    return result.reshape(-1, col_width)


def solution(mesh):
    return jax.shard_map(
        on_device,
        mesh=mesh,
        in_specs=(
            P("dom", "col"),
            P("dom", None, None),
            P(None, "dom"),
            P("dom", None),
            P("dom", None),
            P("dom"),
            P("col", None),
            P("col", None),
        ),
        out_specs=P("dom", "col"),
        check_vma=False,
    )
```

```python
import functools

import jax
import jax.numpy as jnp
from jax import lax
from jax.experimental import pallas as pl
from jax.experimental.pallas import tpu as pltpu
from jax.sharding import PartitionSpec as P

D = 1024
BLOCK_ROWS = 128
CAP = 8
TILES = 32
FAN_T = 4
GROUP = 8
PACK = 16


def aggregate_kernel(
    front, width, slot_of, tile_block, tile_count, nbr_ref, arrived, out_ref, held, turned, nbr_t, sems
):
    step = pl.program_id(0)

    def fetch(p):
        return pltpu.make_async_copy(arrived.at[slot_of[p]], held.at[p], sems.at[p])

    @pl.when(step == 0)
    def _():
        def begin(p, carry):
            fetch(p).start()
            return carry

        lax.fori_loop(0, front, begin, 0)

        def finish(i, carry):
            for k in range(4):
                fetch(i * 4 + k).wait()
            for k in range(4):
                turned[i * 4 + k] = held[i * 4 + k].T
            return carry

        lax.fori_loop(0, front // 4, finish, 0)

    nbr_t[...] = nbr_ref[...].astype(jnp.float32).T
    used = tile_count[step]
    shape = (BLOCK_ROWS // PACK, PACK, BLOCK_ROWS)
    row_ids = (
        lax.broadcasted_iota(jnp.int32, shape, 0) * PACK + lax.broadcasted_iota(jnp.int32, shape, 1)
    ).astype(jnp.float32).astype(jnp.bfloat16)
    one = jnp.ones(shape, jnp.bfloat16)
    zero = jnp.zeros(shape, jnp.bfloat16)

    def body(q, acc):
        nbr = nbr_t[pl.ds(pl.multiple_of(q * (GROUP * FAN_T), GROUP * FAN_T), GROUP * FAN_T), :]
        counts = []
        blocks = []
        for i in range(GROUP):
            tile = q * GROUP + i
            total = None
            for f in range(FAN_T):
                row = nbr[i * FAN_T + f : i * FAN_T + f + 1, :]
                row = jnp.where(tile < used, row, -1.0)
                row = jnp.broadcast_to(row, (PACK, BLOCK_ROWS)).astype(jnp.bfloat16)
                hit = jnp.where(row[None] == row_ids, one, zero)
                total = hit if total is None else total + hit
            counts.append(total.reshape(BLOCK_ROWS, BLOCK_ROWS))
            blocks.append(turned[tile_block[step * TILES + tile]])
        lhs = jnp.concatenate(blocks, axis=1)
        rhs = jnp.concatenate(counts, axis=0)
        return acc + jnp.dot(lhs, rhs, preferred_element_type=jnp.float32)

    summed = lax.fori_loop(
        0, (used + GROUP - 1) // GROUP, body, jnp.zeros((width, BLOCK_ROWS), jnp.float32)
    )
    mean = summed / (used * FAN_T).astype(jnp.float32)
    out_ref[:, :width] = held[step]
    out_ref[:, width:] = mean.T.astype(jnp.bfloat16)


def aggregate(arrived, slot_of, tile_block, local_nbr, tile_count):
    front = slot_of.shape[0]
    width = arrived.shape[-1]
    dst_blocks = tile_count.shape[0]
    return pl.pallas_call(
        functools.partial(aggregate_kernel, front, width),
        out_shape=jax.ShapeDtypeStruct((dst_blocks * BLOCK_ROWS, 2 * width), jnp.bfloat16),
        grid_spec=pltpu.PrefetchScalarGridSpec(
            num_scalar_prefetch=3,
            grid=(dst_blocks,),
            in_specs=[
                pl.BlockSpec((BLOCK_ROWS, TILES * FAN_T), lambda i, *_: (i, 0)),
                pl.BlockSpec(memory_space=pl.ANY),
            ],
            out_specs=pl.BlockSpec((BLOCK_ROWS, 2 * width), lambda i, *_: (i, 0)),
            scratch_shapes=[
                pltpu.VMEM((front, BLOCK_ROWS, width), jnp.bfloat16),
                pltpu.VMEM((front, width, BLOCK_ROWS), jnp.bfloat16),
                pltpu.VMEM((TILES * FAN_T, BLOCK_ROWS), jnp.float32),
                pltpu.SemaphoreType.DMA((front,)),
            ],
        ),
        compiler_params=pltpu.CompilerParams(dimension_semantics=("arbitrary",)),
        cost_estimate=pl.CostEstimate(flops=4 * 10**9, bytes_accessed=8 * 2**20, transcendentals=0),
    )(slot_of, tile_block.reshape(-1), tile_count, local_nbr, arrived)


def project_kernel(n_col, width, order, x_ref, *rest):
    w_refs = rest[:-1]
    out_ref = rest[-1]
    total = None
    for s in range(n_col):
        rows = x_ref[order[s]]
        term = jnp.dot(rows[:, :width], w_refs[2 * s][...], preferred_element_type=jnp.float32)
        term = term + jnp.dot(rows[:, width:], w_refs[2 * s + 1][...], preferred_element_type=jnp.float32)
        total = term if total is None else total + term
    hidden = jnp.maximum(total, 0.0)
    squares = jnp.sum(hidden * hidden, axis=1, keepdims=True)
    result = (hidden / jnp.sqrt(0.25 + squares / D)).astype(jnp.bfloat16)
    for k in range(n_col):
        out_ref[k] = result[:, k * width : (k + 1) * width]


def project(mixed, weights, order):
    n_col, rows, _ = mixed.shape
    width = D // n_col
    tile = BLOCK_ROWS
    return pl.pallas_call(
        functools.partial(project_kernel, n_col, width),
        out_shape=jax.ShapeDtypeStruct((n_col, rows, width), jnp.bfloat16),
        grid_spec=pltpu.PrefetchScalarGridSpec(
            num_scalar_prefetch=1,
            grid=(rows // tile,),
            in_specs=[pl.BlockSpec((n_col, tile, 2 * width), lambda i, *_: (0, i, 0))]
            + [pl.BlockSpec((width, D), lambda i, *_: (0, 0)) for _ in weights],
            out_specs=pl.BlockSpec((n_col, tile, width), lambda i, *_: (0, i, 0)),
        ),
        compiler_params=pltpu.CompilerParams(dimension_semantics=("arbitrary",)),
        cost_estimate=pl.CostEstimate(flops=2 * 10**9, bytes_accessed=7 * 2**20, transcendentals=0),
    )(order, mixed, *weights)


MESH = pl.DeviceIdType.MESH
PARTS = 2
PAIR = 2
EARLY_LAG = 4
NEAR_LAG = 2
SWAP_LAG = 5
SUM_LAG = 8
LINE = 4


def exchange_kernel(n_dom, outgoing, arrived, send, recv, own_sem):
    me = lax.axis_index("dom")

    def copy_to(d):
        peer = lax.rem(me + d, n_dom)
        return pltpu.make_async_remote_copy(
            src_ref=outgoing.at[peer], dst_ref=arrived.at[me], send_sem=send.at[d], recv_sem=recv.at[d],
            device_id={"dom": peer}, device_id_type=MESH,
        )

    own = pltpu.make_async_copy(outgoing.at[me], arrived.at[me], own_sem)
    for d in range(1, n_dom):
        copy_to(d).start()
    own.start()
    own.wait()
    for d in range(1, n_dom):
        copy_to(d).wait_send()
        copy_to(d).wait_recv()


def exchange(outgoing):
    n_dom = outgoing.shape[0]
    anywhere = pl.BlockSpec(memory_space=pl.ANY)
    return pl.pallas_call(
        functools.partial(exchange_kernel, n_dom),
        out_shape=jax.ShapeDtypeStruct(outgoing.shape, outgoing.dtype),
        in_specs=[anywhere],
        out_specs=anywhere,
        scratch_shapes=[
            pltpu.SemaphoreType.DMA((n_dom,)),
            pltpu.SemaphoreType.DMA((n_dom,)),
            pltpu.SemaphoreType.DMA,
        ],
        compiler_params=pltpu.CompilerParams(has_side_effects=True),
    )(outgoing)


def line_kernel(
    n_dom, requests_in, counts_in, tile_block_in, tile_count_in, features, local_nbr, w_self, w_neigh, out,
    feat, outgoing, arrived_early, arrived_late, nbr_in, nbr_t, hits, mixed, near, part, part_in, kept_theirs, kept_mine, sums, sums_in, passed, passed_in,
    own_w, far_w, turned_w, result, requests, counts, tile_block, tile_count, slot_of,
    load_sem, own_sem, send, recv, w_send, w_recv, swap_send, swap_recv, store_sem,
    near_send, near_recv, part_send, part_recv, out_send, out_recv, sum_send, sum_recv,
):
    me = lax.axis_index("dom")
    z = lax.axis_index("col")
    core = lax.rem(me, 2)
    chip = me // 2
    n_chip = n_dom // 2
    front = slot_of.shape[0]
    _, dst_blocks, width, _ = mixed.shape
    span = 2 * width
    piece = width // PARTS
    at_end = jnp.logical_or(z == 0, z == LINE - 1)
    inside = jnp.logical_not(at_end)
    half = z // 2

    arrived = (arrived_early, arrived_late)

    def remote(src, dst, s_sem, r_sem, **device):
        return pltpu.make_async_remote_copy(
            src_ref=src, dst_ref=dst, send_sem=s_sem, recv_sem=r_sem, device_id=device, device_id_type=MESH,
        )

    loads = [
        pltpu.make_async_copy(src, dst, load_sem.at[i])
        for i, (src, dst) in enumerate(
            (
                (requests_in, requests),
                (features, feat),
                (counts_in, counts),
                (tile_count_in, tile_count),
                (tile_block_in, tile_block),
                (w_self, own_w.at[0]),
                (w_neigh, own_w.at[1]),
                (local_nbr, nbr_in),
            )
        )
    ]
    for copy in loads:
        copy.start()

    barrier = pltpu.get_barrier_semaphore()

    def greet(d, carry):
        pl.semaphore_signal(barrier, inc=1, device_id={"dom": lax.rem(me + d, n_dom)}, device_id_type=MESH)
        return carry

    lax.fori_loop(1, n_dom, greet, 0)

    for inner in (1, 2):

        @pl.when(z != inner)
        def _(inner=inner):
            pl.semaphore_signal(barrier, inc=1, device_id={"col": inner}, device_id_type=MESH)

    @pl.when(inside)
    def _():
        pl.semaphore_signal(barrier, inc=1, device_id={"col": 0}, device_id_type=MESH)
        pl.semaphore_signal(barrier, inc=1, device_id={"col": LINE - 1}, device_id_type=MESH)
        pl.semaphore_wait(barrier, n_dom + 2)

    @pl.when(at_end)
    def _():
        pl.semaphore_wait(barrier, n_dom + 1)

    def weight_copy():
        return remote(own_w.at[core], far_w.at[core], w_send, w_recv, col=1 + half)

    def swap_copy(which):
        return remote(far_w.at[which], far_w.at[which], swap_send, swap_recv, dom=me + 1 - 2 * core)

    def slots(owner):
        return pl.ds(owner * CAP, CAP)

    def block_copy(k, peer, owner):
        return remote(
            outgoing.at[k, slots(peer)], arrived[k].at[slots(owner)], send.at[k, peer], recv.at[k, owner], dom=peer
        )

    def own_copy(k):
        return pltpu.make_async_copy(outgoing.at[k, slots(me)], arrived[k].at[slots(me)], own_sem.at[k])

    loads[0].wait()
    loads[1].wait()

    def peer_of(group, turn):
        if n_chip == 4:
            column = lax.rem(chip, 2)
            toward = jnp.where(
                turn == 0, 3 - chip,
                jnp.where(turn == 1, lax.rem(chip + 2, 4), jnp.where(turn == 2, chip + 1 - 2 * column, chip)),
            )
        else:
            toward = lax.rem(chip + 1 + turn, n_chip)
        return toward * 2 + group

    def give(k, peer):
        @pl.when(peer == me)
        def _():
            own_copy(k).start()

        @pl.when(peer != me)
        def _():
            block_copy(k, peer, me).start()

    for group in range(2):

        def pick(turn, carry, group=group):
            peer = peer_of(group, turn)
            for s in range(CAP):
                block = feat[requests[0, peer, s]].T
                for k in range(PARTS):
                    outgoing[k, peer * CAP + s] = block[k * piece : (k + 1) * piece]
            give(0, peer)
            return carry

        lax.fori_loop(0, n_chip, pick, 0)
        for k in range(1, PARTS):

            def later(turn, carry, group=group, k=k):
                give(k, peer_of(group, turn))
                return carry

            lax.fori_loop(0, n_chip, later, 0)

    for copy in loads[2:]:
        copy.wait()

    @pl.when(at_end)
    def _():
        weight_copy().start()

    ends = []
    end = jnp.int32(0)
    for o in range(n_dom):
        end = end + counts[o]
        ends.append(end)

    def place(p, carry):
        owner = jnp.int32(0)
        start = jnp.int32(0)
        for o in range(n_dom):
            passed_by = ends[o] <= p
            owner = owner + jnp.where(passed_by, 1, 0)
            start = jnp.where(passed_by, ends[o], start)
        slot_of[p] = jnp.minimum(owner * CAP + p - start, n_dom * CAP - 1)
        return carry

    lax.fori_loop(0, front, place, 0)

    shape = (BLOCK_ROWS // PACK, PACK, BLOCK_ROWS)
    row_ids = (
        lax.broadcasted_iota(jnp.int32, shape, 0) * PACK + lax.broadcasted_iota(jnp.int32, shape, 1)
    ).astype(jnp.float32).astype(jnp.bfloat16)
    one = jnp.ones(shape, jnp.bfloat16)
    zero = jnp.zeros(shape, jnp.bfloat16)
    sample = lax.broadcasted_iota(jnp.int32, (TILES * FAN_T, BLOCK_ROWS), 0)
    groups = TILES // GROUP

    def prepare(b, carry):
        picked = nbr_in[pl.ds(pl.multiple_of(b * BLOCK_ROWS, BLOCK_ROWS), BLOCK_ROWS), :].astype(jnp.float32).T
        nbr_t[...] = jnp.where(sample < tile_count[b] * FAN_T, picked, -1.0)

        def build(q, inner):
            nbr = nbr_t[pl.ds(pl.multiple_of(q * (GROUP * FAN_T), GROUP * FAN_T), GROUP * FAN_T), :]
            for i in range(GROUP):
                total = None
                for f in range(FAN_T):
                    row = nbr[i * FAN_T + f : i * FAN_T + f + 1, :]
                    row = jnp.broadcast_to(row, (PACK, BLOCK_ROWS)).astype(jnp.bfloat16)
                    hit = jnp.where(row[None] == row_ids, one, zero)
                    total = hit if total is None else total + hit
                hits[b * groups + q, i * BLOCK_ROWS : (i + 1) * BLOCK_ROWS, :] = total.reshape(BLOCK_ROWS, BLOCK_ROWS)
            return inner

        return lax.fori_loop(0, groups, build, carry)

    lax.fori_loop(0, dst_blocks, prepare, 0)

    @pl.when(inside)
    def _():
        weight_copy().wait_recv()
        swap_copy(core).start()

        def turn_weights(source, base):
            for h in range(2):
                rank = jnp.where(half == h, 1, 0)
                for i in range(2):
                    turned = source[i, :, h * span : (h + 1) * span].T
                    for k in range(PARTS):
                        columns = slice(base + i * piece, base + (i + 1) * piece)
                        turned_w[k, rank, :, columns] = turned[:, k * piece : (k + 1) * piece]

        turn_weights(own_w, 0)
        swap_copy(1 - core).wait_recv()
        turn_weights(far_w, width)

    def take(k):
        own_copy(k).wait()

        def one_owner(d, carry):
            owner = lax.rem(me + d, n_dom)
            block_copy(k, owner, owner).wait_recv()
            return carry

        lax.fori_loop(1, n_dom, one_owner, 0)

    def near_copy(k, c):
        return remote(mixed.at[k, c], near.at[k, c], near_send.at[k, c], near_recv.at[k, c], col=1 + half)

    def part_copy(c):
        return remote(part.at[c], part_in.at[c], part_send.at[c], part_recv.at[c], col=2 - half)

    def sum_copy(c, k):
        target = (2 - half, half * (LINE - 1), (1 - half) * (LINE - 1))[k]
        return remote(sums.at[c], sums_in.at[k, c], sum_send.at[k, c], sum_recv.at[k, c], col=target)

    def out_copy(c):
        return remote(passed.at[c], passed_in.at[c], out_send.at[c], out_recv.at[c], col=half * (LINE - 1))

    def store_copy(c):
        rows = pl.ds(pl.multiple_of(c * BLOCK_ROWS, BLOCK_ROWS), BLOCK_ROWS)
        return pltpu.make_async_copy(result.at[c], out.at[rows], store_sem.at[c])

    def emit(c, hidden, squares):
        scale = 1.0 / jnp.sqrt(0.25 + squares / D)
        result[c] = (hidden * scale).astype(jnp.bfloat16).T
        store_copy(c).start()

    def gather(k, b):
        used = tile_count[b]
        summed = None
        for q in range(groups):
            blocks = [arrived[k][slot_of[tile_block[b, q * GROUP + i]]] for i in range(GROUP)]
            term = jnp.dot(
                jnp.concatenate(blocks, axis=1), hits[b * groups + q], preferred_element_type=jnp.float32
            )
            summed = term if summed is None else summed + term
        mean = summed / (used * FAN_T).astype(jnp.float32)
        mixed[k, b, :piece] = arrived[k][slot_of[b]]
        mixed[k, b, piece:] = mean.astype(jnp.bfloat16)

    def product(k, blocks):
        weights = turned_w[k].reshape(2 * span, span)
        rhs = jnp.concatenate(
            [jnp.concatenate([mixed[k, c] for c in blocks], axis=1), jnp.concatenate([near[k, c] for c in blocks], axis=1)],
            axis=0,
        )
        return jnp.dot(weights, rhs, preferred_element_type=jnp.float32)

    def early(i):
        blocks = [i * PAIR + j for j in range(PAIR)]
        for c in blocks:
            near_copy(0, c).wait_recv()
        total = product(0, blocks)
        for j, c in enumerate(blocks):
            kept_theirs[c] = total[:span, j * BLOCK_ROWS : (j + 1) * BLOCK_ROWS]
            kept_mine[c] = total[span:, j * BLOCK_ROWS : (j + 1) * BLOCK_ROWS]

    def first(c):
        near_copy(1, c).wait_recv()
        total = product(1, [c])
        part[c] = (kept_theirs[c] + total[:span]).astype(jnp.bfloat16)
        part_copy(c).start()
        kept_mine[c] = kept_mine[c] + total[span:]

    def second(c):
        part_copy(c).wait_recv()
        hidden = jnp.maximum(kept_mine[c] + part_in[c].astype(jnp.float32), 0.0)
        sums[c] = jnp.sum(hidden * hidden, axis=0, keepdims=True)
        low, high = hidden[:width], hidden[width:]
        passed[c] = jnp.where(half == 0, low, high).astype(jnp.bfloat16)
        for k in range(3):
            sum_copy(c, k).start()
        out_copy(c).start()
        kept_mine[c, :width] = jnp.where(half == 0, high, low)

    def third(c):
        sum_copy(c, 0).wait_recv()
        emit(c, kept_mine[c, :width], sums[c] + sums_in[0, c])

    take(0)

    @pl.when(at_end)
    def _():
        def send_early(c, carry):
            gather(0, c)
            near_copy(0, c).start()
            return carry

        lax.fori_loop(0, dst_blocks, send_early, 0)

    pairs = dst_blocks // PAIR

    @pl.when(inside)
    def _():
        def prelude(i, carry):
            for j in range(PAIR):
                gather(0, i * PAIR + j)

            @pl.when(i >= EARLY_LAG)
            def _():
                early(i - EARLY_LAG)

            return carry

        lax.fori_loop(0, pairs, prelude, 0)

    take(1)

    @pl.when(at_end)
    def _():
        def send_late(c, carry):
            gather(1, c)
            near_copy(1, c).start()
            return carry

        lax.fori_loop(0, dst_blocks, send_late, 0)

        def receive(c, carry):
            out_copy(c).wait_recv()
            sum_copy(c, 1).wait_recv()
            sum_copy(c, 2).wait_recv()
            emit(c, passed_in[c].astype(jnp.float32), sums_in[1, c] + sums_in[2, c])
            for k in range(PARTS):
                near_copy(k, c).wait_send()
            return carry

        lax.fori_loop(0, dst_blocks, receive, 0)
        weight_copy().wait_send()

    @pl.when(inside)
    def _():
        def late(c):
            gather(1, c)

        def stage(i, carry):
            due = i - NEAR_LAG + 1

            @pl.when(jnp.logical_and(jnp.logical_and(due >= (pairs - EARLY_LAG) * PAIR, due < dst_blocks), due % PAIR == 0))
            def _():
                early(due // PAIR)

            for lag, work in ((0, late), (NEAR_LAG, first), (SWAP_LAG, second), (SUM_LAG, third)):

                @pl.when(jnp.logical_and(i >= lag, i < dst_blocks + lag))
                def _(lag=lag, work=work):
                    work(i - lag)

            return carry

        lax.fori_loop(0, dst_blocks + SUM_LAG, stage, 0)

        def finish(c, carry):
            part_copy(c).wait_send()
            for k in range(3):
                sum_copy(c, k).wait_send()
            out_copy(c).wait_send()
            return carry

        lax.fori_loop(0, dst_blocks, finish, 0)
        swap_copy(core).wait_send()

    def stored(c, carry):
        store_copy(c).wait()
        return carry

    lax.fori_loop(0, dst_blocks, stored, 0)

    def sent(d, carry):
        peer = lax.rem(me + d, n_dom)
        for k in range(PARTS):
            block_copy(k, peer, me).wait_send()
        return carry

    lax.fori_loop(1, n_dom, sent, 0)


def on_line(features, requests, counts, tile_block, local_nbr, tile_count, w_self, w_neigh):
    n_dom = lax.axis_size("dom")
    total, width = local_nbr.shape[0], features.shape[1]
    dst_blocks = total // BLOCK_ROWS
    span = 2 * width
    blocks = features.reshape(-1, BLOCK_ROWS, width)
    anywhere = pl.BlockSpec(memory_space=pl.ANY)
    dma = pltpu.SemaphoreType.DMA
    bf16, f32 = jnp.bfloat16, jnp.float32
    return pl.pallas_call(
        functools.partial(line_kernel, n_dom),
        out_shape=jax.ShapeDtypeStruct((total, width), bf16),
        in_specs=[anywhere] * 8,
        out_specs=anywhere,
        scratch_shapes=[
            pltpu.VMEM(blocks.shape, bf16),
            pltpu.VMEM((PARTS, n_dom * CAP, width // PARTS, BLOCK_ROWS), bf16),
            pltpu.VMEM((n_dom * CAP, width // PARTS, BLOCK_ROWS), bf16),
            pltpu.VMEM((n_dom * CAP, width // PARTS, BLOCK_ROWS), bf16),
            pltpu.VMEM(local_nbr.shape, jnp.int32),
            pltpu.VMEM((TILES * FAN_T, BLOCK_ROWS), f32),
            pltpu.VMEM((dst_blocks * TILES // GROUP, GROUP * BLOCK_ROWS, BLOCK_ROWS), bf16),
            pltpu.VMEM((PARTS, dst_blocks, span // PARTS, BLOCK_ROWS), bf16),
            pltpu.VMEM((PARTS, dst_blocks, span // PARTS, BLOCK_ROWS), bf16),
            pltpu.VMEM((dst_blocks, span, BLOCK_ROWS), bf16),
            pltpu.VMEM((dst_blocks, span, BLOCK_ROWS), bf16),
            pltpu.VMEM((dst_blocks, span, BLOCK_ROWS), f32),
            pltpu.VMEM((dst_blocks, span, BLOCK_ROWS), f32),
            pltpu.VMEM((dst_blocks, 1, BLOCK_ROWS), f32),
            pltpu.VMEM((3, dst_blocks, 1, BLOCK_ROWS), f32),
            pltpu.VMEM((dst_blocks, width, BLOCK_ROWS), bf16),
            pltpu.VMEM((dst_blocks, width, BLOCK_ROWS), bf16),
            pltpu.VMEM((2,) + w_self.shape, bf16),
            pltpu.VMEM((2,) + w_self.shape, bf16),
            pltpu.VMEM((PARTS, 2, span, 2 * span // PARTS), bf16),
            pltpu.VMEM((dst_blocks, BLOCK_ROWS, width), bf16),
            pltpu.SMEM(requests.shape, jnp.int32),
            pltpu.SMEM(counts.shape[:1], jnp.int32),
            pltpu.SMEM(tile_block.shape, jnp.int32),
            pltpu.SMEM(tile_count.shape, jnp.int32),
            pltpu.SMEM((n_dom * CAP // 2,), jnp.int32),
            dma((8,)), dma((PARTS,)), dma((PARTS, n_dom)), dma((PARTS, n_dom)), dma, dma, dma, dma, dma((dst_blocks,)),
        ]
        + [dma((PARTS, dst_blocks))] * 2
        + [dma((dst_blocks,))] * 4
        + [dma((3, dst_blocks))] * 2,
        compiler_params=pltpu.CompilerParams(has_side_effects=True, collective_id=0, vmem_limit_bytes=67_000_000),
    )(requests, counts.reshape(-1), tile_block, tile_count, blocks, local_nbr, w_self, w_neigh)


def on_device(features, requests, counts, tile_block, local_nbr, tile_count, w_self, w_neigh):
    n_dom = lax.axis_size("dom")
    n_col = lax.axis_size("col")
    col_width = features.shape[1]
    if n_col == LINE:
        return on_line(features, requests, counts, tile_block, local_nbr, tile_count, w_self, w_neigh)
    blocks = features.reshape(-1, BLOCK_ROWS, col_width)
    outgoing = blocks.at[requests[0].reshape(-1)].get(mode="promise_in_bounds")
    outgoing = outgoing.reshape(n_dom, CAP, BLOCK_ROWS, col_width)
    arrived = exchange(outgoing).reshape(n_dom * CAP, BLOCK_ROWS, col_width)
    slot_ends = jnp.cumsum(counts[:, 0])
    positions = jnp.arange(n_dom * CAP // 2, dtype=jnp.int32)
    passed = slot_ends[None, :] <= positions[:, None]
    owner_of = jnp.sum(passed.astype(jnp.int32), axis=1)
    start_of = jnp.max(jnp.where(passed, slot_ends[None, :], 0), axis=1)
    slot_of = owner_of * CAP + positions - start_of

    mixed = aggregate(arrived, slot_of, tile_block, local_nbr, tile_count)
    weights = [w_self, w_neigh]
    for shift in range(1, n_col):
        perm = [(k, (k + shift) % n_col) for k in range(n_col)]
        weights.append(lax.ppermute(w_self, "col", perm))
        weights.append(lax.ppermute(w_neigh, "col", perm))
    order = (lax.axis_index("col") - jnp.arange(n_col, dtype=jnp.int32)) % n_col
    mixed = mixed.reshape(n_col, -1, 2 * col_width)
    mixed = lax.all_to_all(mixed, "col", split_axis=0, concat_axis=0, tiled=True)
    result = project(mixed, weights, order)
    result = lax.all_to_all(result, "col", split_axis=0, concat_axis=0, tiled=True)
    return result.reshape(-1, col_width)


def solution(mesh):
    return jax.shard_map(
        on_device,
        mesh=mesh,
        in_specs=(
            P("dom", "col"),
            P("dom", None, None),
            P(None, "dom"),
            P("dom", None),
            P("dom", None),
            P("dom"),
            P("col", None),
            P("col", None),
        ),
        out_specs=P("dom", "col"),
        check_vma=False,
    )
```

```python
import functools

import jax
import jax.numpy as jnp
from jax import lax
from jax.experimental import pallas as pl
from jax.experimental.pallas import tpu as pltpu
from jax.sharding import PartitionSpec as P

D = 1024
BLOCK_ROWS = 128
CAP = 8
TILES = 32
FAN_T = 4
GROUP = 8
PACK = 16


def aggregate_kernel(
    front, width, slot_of, tile_block, tile_count, nbr_ref, arrived, out_ref, held, turned, nbr_t, sems
):
    step = pl.program_id(0)

    def fetch(p):
        return pltpu.make_async_copy(arrived.at[slot_of[p]], held.at[p], sems.at[p])

    @pl.when(step == 0)
    def _():
        def begin(p, carry):
            fetch(p).start()
            return carry

        lax.fori_loop(0, front, begin, 0)

        def finish(i, carry):
            for k in range(4):
                fetch(i * 4 + k).wait()
            for k in range(4):
                turned[i * 4 + k] = held[i * 4 + k].T
            return carry

        lax.fori_loop(0, front // 4, finish, 0)

    nbr_t[...] = nbr_ref[...].astype(jnp.float32).T
    used = tile_count[step]
    shape = (BLOCK_ROWS // PACK, PACK, BLOCK_ROWS)
    row_ids = (
        lax.broadcasted_iota(jnp.int32, shape, 0) * PACK + lax.broadcasted_iota(jnp.int32, shape, 1)
    ).astype(jnp.float32).astype(jnp.bfloat16)
    one = jnp.ones(shape, jnp.bfloat16)
    zero = jnp.zeros(shape, jnp.bfloat16)

    def body(q, acc):
        nbr = nbr_t[pl.ds(pl.multiple_of(q * (GROUP * FAN_T), GROUP * FAN_T), GROUP * FAN_T), :]
        counts = []
        blocks = []
        for i in range(GROUP):
            tile = q * GROUP + i
            total = None
            for f in range(FAN_T):
                row = nbr[i * FAN_T + f : i * FAN_T + f + 1, :]
                row = jnp.where(tile < used, row, -1.0)
                row = jnp.broadcast_to(row, (PACK, BLOCK_ROWS)).astype(jnp.bfloat16)
                hit = jnp.where(row[None] == row_ids, one, zero)
                total = hit if total is None else total + hit
            counts.append(total.reshape(BLOCK_ROWS, BLOCK_ROWS))
            blocks.append(turned[tile_block[step * TILES + tile]])
        lhs = jnp.concatenate(blocks, axis=1)
        rhs = jnp.concatenate(counts, axis=0)
        return acc + jnp.dot(lhs, rhs, preferred_element_type=jnp.float32)

    summed = lax.fori_loop(
        0, (used + GROUP - 1) // GROUP, body, jnp.zeros((width, BLOCK_ROWS), jnp.float32)
    )
    mean = summed / (used * FAN_T).astype(jnp.float32)
    out_ref[:, :width] = held[step]
    out_ref[:, width:] = mean.T.astype(jnp.bfloat16)


def aggregate(arrived, slot_of, tile_block, local_nbr, tile_count):
    front = slot_of.shape[0]
    width = arrived.shape[-1]
    dst_blocks = tile_count.shape[0]
    return pl.pallas_call(
        functools.partial(aggregate_kernel, front, width),
        out_shape=jax.ShapeDtypeStruct((dst_blocks * BLOCK_ROWS, 2 * width), jnp.bfloat16),
        grid_spec=pltpu.PrefetchScalarGridSpec(
            num_scalar_prefetch=3,
            grid=(dst_blocks,),
            in_specs=[
                pl.BlockSpec((BLOCK_ROWS, TILES * FAN_T), lambda i, *_: (i, 0)),
                pl.BlockSpec(memory_space=pl.ANY),
            ],
            out_specs=pl.BlockSpec((BLOCK_ROWS, 2 * width), lambda i, *_: (i, 0)),
            scratch_shapes=[
                pltpu.VMEM((front, BLOCK_ROWS, width), jnp.bfloat16),
                pltpu.VMEM((front, width, BLOCK_ROWS), jnp.bfloat16),
                pltpu.VMEM((TILES * FAN_T, BLOCK_ROWS), jnp.float32),
                pltpu.SemaphoreType.DMA((front,)),
            ],
        ),
        compiler_params=pltpu.CompilerParams(dimension_semantics=("arbitrary",)),
        cost_estimate=pl.CostEstimate(flops=4 * 10**9, bytes_accessed=8 * 2**20, transcendentals=0),
    )(slot_of, tile_block.reshape(-1), tile_count, local_nbr, arrived)


def project_kernel(n_col, width, order, x_ref, *rest):
    w_refs = rest[:-1]
    out_ref = rest[-1]
    total = None
    for s in range(n_col):
        rows = x_ref[order[s]]
        term = jnp.dot(rows[:, :width], w_refs[2 * s][...], preferred_element_type=jnp.float32)
        term = term + jnp.dot(rows[:, width:], w_refs[2 * s + 1][...], preferred_element_type=jnp.float32)
        total = term if total is None else total + term
    hidden = jnp.maximum(total, 0.0)
    squares = jnp.sum(hidden * hidden, axis=1, keepdims=True)
    result = (hidden / jnp.sqrt(0.25 + squares / D)).astype(jnp.bfloat16)
    for k in range(n_col):
        out_ref[k] = result[:, k * width : (k + 1) * width]


def project(mixed, weights, order):
    n_col, rows, _ = mixed.shape
    width = D // n_col
    tile = BLOCK_ROWS
    return pl.pallas_call(
        functools.partial(project_kernel, n_col, width),
        out_shape=jax.ShapeDtypeStruct((n_col, rows, width), jnp.bfloat16),
        grid_spec=pltpu.PrefetchScalarGridSpec(
            num_scalar_prefetch=1,
            grid=(rows // tile,),
            in_specs=[pl.BlockSpec((n_col, tile, 2 * width), lambda i, *_: (0, i, 0))]
            + [pl.BlockSpec((width, D), lambda i, *_: (0, 0)) for _ in weights],
            out_specs=pl.BlockSpec((n_col, tile, width), lambda i, *_: (0, i, 0)),
        ),
        compiler_params=pltpu.CompilerParams(dimension_semantics=("arbitrary",)),
        cost_estimate=pl.CostEstimate(flops=2 * 10**9, bytes_accessed=7 * 2**20, transcendentals=0),
    )(order, mixed, *weights)


MESH = pl.DeviceIdType.MESH
PARTS = 2
PAIR = 2
EARLY_LAG = 6
NEAR_LAG = 3
SWAP_LAG = 6
SUM_LAG = 9
LINE = 4
DELIVER = 2


def exchange_kernel(n_dom, outgoing, arrived, send, recv, own_sem):
    me = lax.axis_index("dom")

    def copy_to(d):
        peer = lax.rem(me + d, n_dom)
        return pltpu.make_async_remote_copy(
            src_ref=outgoing.at[peer], dst_ref=arrived.at[me], send_sem=send.at[d], recv_sem=recv.at[d],
            device_id={"dom": peer}, device_id_type=MESH,
        )

    own = pltpu.make_async_copy(outgoing.at[me], arrived.at[me], own_sem)
    for d in range(1, n_dom):
        copy_to(d).start()
    own.start()
    own.wait()
    for d in range(1, n_dom):
        copy_to(d).wait_send()
        copy_to(d).wait_recv()


def exchange(outgoing):
    n_dom = outgoing.shape[0]
    anywhere = pl.BlockSpec(memory_space=pl.ANY)
    return pl.pallas_call(
        functools.partial(exchange_kernel, n_dom),
        out_shape=jax.ShapeDtypeStruct(outgoing.shape, outgoing.dtype),
        in_specs=[anywhere],
        out_specs=anywhere,
        scratch_shapes=[
            pltpu.SemaphoreType.DMA((n_dom,)),
            pltpu.SemaphoreType.DMA((n_dom,)),
            pltpu.SemaphoreType.DMA,
        ],
        compiler_params=pltpu.CompilerParams(has_side_effects=True),
    )(outgoing)


def line_kernel(
    n_dom, requests_in, counts_in, tile_block_in, tile_count_in, features, local_nbr, w_self, w_neigh, out,
    feat, outgoing, arrived_early, arrived_late, nbr_in, nbr_t, hits, mixed, near, part, part_in, kept_theirs, kept_mine, sums, sums_in, passed, passed_in,
    own_w, far_w, turned_w, requests, counts, tile_block, tile_count, slot_of,
    load_sem, own_sem, send, recv, w_send, w_recv, swap_send, swap_recv,
    near_send, near_recv, part_send, part_recv, out_send, out_recv, sum_send, sum_recv,
):
    me = lax.axis_index("dom")
    z = lax.axis_index("col")
    core = lax.rem(me, 2)
    chip = me // 2
    n_chip = n_dom // 2
    front = slot_of.shape[0]
    _, dst_blocks, width, _ = mixed.shape
    span = 2 * width
    piece = width // PARTS
    at_end = jnp.logical_or(z == 0, z == LINE - 1)
    inside = jnp.logical_not(at_end)
    half = z // 2

    arrived = (arrived_early, arrived_late)

    def remote(src, dst, s_sem, r_sem, **device):
        return pltpu.make_async_remote_copy(
            src_ref=src, dst_ref=dst, send_sem=s_sem, recv_sem=r_sem, device_id=device, device_id_type=MESH,
        )

    loads = [
        pltpu.make_async_copy(src, dst, load_sem.at[i])
        for i, (src, dst) in enumerate(
            (
                (requests_in, requests),
                (features, feat),
                (counts_in, counts),
                (tile_count_in, tile_count),
                (tile_block_in, tile_block),
                (w_self, own_w.at[0]),
                (w_neigh, own_w.at[1]),
                (local_nbr, nbr_in),
            )
        )
    ]
    for copy in loads:
        copy.start()

    barrier = pltpu.get_barrier_semaphore()

    def greet(d, carry):
        pl.semaphore_signal(barrier, inc=1, device_id={"dom": lax.rem(me + d, n_dom)}, device_id_type=MESH)
        return carry

    lax.fori_loop(1, n_dom, greet, 0)

    for inner in (1, 2):

        @pl.when(z != inner)
        def _(inner=inner):
            pl.semaphore_signal(barrier, inc=1, device_id={"col": inner}, device_id_type=MESH)

    @pl.when(inside)
    def _():
        pl.semaphore_signal(barrier, inc=1, device_id={"col": 0}, device_id_type=MESH)
        pl.semaphore_signal(barrier, inc=1, device_id={"col": LINE - 1}, device_id_type=MESH)
        pl.semaphore_wait(barrier, n_dom + 2)

    @pl.when(at_end)
    def _():
        pl.semaphore_wait(barrier, n_dom + 1)

    def weight_copy():
        return remote(own_w.at[core], far_w.at[core], w_send, w_recv, col=1 + half)

    def swap_copy(which):
        return remote(far_w.at[which], far_w.at[which], swap_send, swap_recv, dom=me + 1 - 2 * core)

    def slots(owner):
        return pl.ds(owner * CAP, CAP)

    def block_copy(k, peer, owner):
        return remote(
            outgoing.at[k, slots(peer)], arrived[k].at[slots(owner)], send.at[k, peer], recv.at[k, owner], dom=peer
        )

    def own_copy(k):
        return pltpu.make_async_copy(outgoing.at[k, slots(me)], arrived[k].at[slots(me)], own_sem.at[k])

    loads[0].wait()
    loads[1].wait()

    def peer_of(group, turn):
        if n_chip == 4:
            column = lax.rem(chip, 2)
            toward = jnp.where(
                turn == 0, 3 - chip,
                jnp.where(turn == 1, lax.rem(chip + 2, 4), jnp.where(turn == 2, chip + 1 - 2 * column, chip)),
            )
        else:
            toward = lax.rem(chip + 1 + turn, n_chip)
        return toward * 2 + group

    def give(k, peer):
        @pl.when(peer == me)
        def _():
            own_copy(k).start()

        @pl.when(peer != me)
        def _():
            block_copy(k, peer, me).start()

    for group in range(2):

        def pick(turn, carry, group=group):
            peer = peer_of(group, turn)
            for s in range(CAP):
                block = feat[requests[0, peer, s]].T
                for k in range(PARTS):
                    outgoing[k, peer * CAP + s] = block[k * piece : (k + 1) * piece]
            give(0, peer)
            return carry

        lax.fori_loop(0, n_chip, pick, 0)
        for k in range(1, PARTS):

            def later(turn, carry, group=group, k=k):
                give(k, peer_of(group, turn))
                return carry

            lax.fori_loop(0, n_chip, later, 0)

    for copy in loads[2:]:
        copy.wait()

    @pl.when(at_end)
    def _():
        weight_copy().start()

    ends = []
    end = jnp.int32(0)
    for o in range(n_dom):
        end = end + counts[o]
        ends.append(end)

    def place(p, carry):
        owner = jnp.int32(0)
        start = jnp.int32(0)
        for o in range(n_dom):
            passed_by = ends[o] <= p
            owner = owner + jnp.where(passed_by, 1, 0)
            start = jnp.where(passed_by, ends[o], start)
        slot_of[p] = jnp.minimum(owner * CAP + p - start, n_dom * CAP - 1)
        return carry

    lax.fori_loop(0, front, place, 0)

    shape = (BLOCK_ROWS // PACK, PACK, BLOCK_ROWS)
    row_ids = (
        lax.broadcasted_iota(jnp.int32, shape, 0) * PACK + lax.broadcasted_iota(jnp.int32, shape, 1)
    ).astype(jnp.float32).astype(jnp.bfloat16)
    one = jnp.ones(shape, jnp.bfloat16)
    zero = jnp.zeros(shape, jnp.bfloat16)
    sample = lax.broadcasted_iota(jnp.int32, (TILES * FAN_T, BLOCK_ROWS), 0)
    groups = TILES // GROUP

    def prepare(b, carry):
        picked = nbr_in[pl.ds(pl.multiple_of(b * BLOCK_ROWS, BLOCK_ROWS), BLOCK_ROWS), :].astype(jnp.float32).T
        nbr_t[...] = jnp.where(sample < tile_count[b] * FAN_T, picked, -1.0)

        def build(q, inner):
            nbr = nbr_t[pl.ds(pl.multiple_of(q * (GROUP * FAN_T), GROUP * FAN_T), GROUP * FAN_T), :]
            for i in range(GROUP):
                total = None
                for f in range(FAN_T):
                    row = nbr[i * FAN_T + f : i * FAN_T + f + 1, :]
                    row = jnp.broadcast_to(row, (PACK, BLOCK_ROWS)).astype(jnp.bfloat16)
                    hit = jnp.where(row[None] == row_ids, one, zero)
                    total = hit if total is None else total + hit
                hits[b * groups + q, i * BLOCK_ROWS : (i + 1) * BLOCK_ROWS, :] = total.reshape(BLOCK_ROWS, BLOCK_ROWS)
            return inner

        return lax.fori_loop(0, groups, build, carry)

    lax.fori_loop(0, dst_blocks, prepare, 0)

    @pl.when(inside)
    def _():
        weight_copy().wait_recv()
        swap_copy(core).start()

        def turn_weights(source, base):
            for h in range(2):
                rank = jnp.where(half == h, 1, 0)
                for i in range(2):
                    turned = source[i, :, h * span : (h + 1) * span].T
                    for k in range(PARTS):
                        columns = slice(base + i * piece, base + (i + 1) * piece)
                        turned_w[k, rank, :, columns] = turned[:, k * piece : (k + 1) * piece]

        turn_weights(own_w, 0)
        swap_copy(1 - core).wait_recv()
        turn_weights(far_w, width)

    def take(k):
        own_copy(k).wait()

        def one_owner(d, carry):
            owner = lax.rem(me + d, n_dom)
            block_copy(k, owner, owner).wait_recv()
            return carry

        lax.fori_loop(1, n_dom, one_owner, 0)

    def near_copy(k, c):
        return remote(mixed.at[k, c], near.at[k, c], near_send.at[k, c], near_recv.at[k, c], col=1 + half)

    def part_copy(c):
        return remote(part.at[c], part_in.at[c], part_send.at[c], part_recv.at[c], col=2 - half)

    def sum_copy(c, k):
        target = (2 - half, half * (LINE - 1), (1 - half) * (LINE - 1))[k]
        return remote(sums.at[c], sums_in.at[k, c], sum_send.at[k, c], sum_recv.at[k, c], col=target)

    def out_copy(c):
        return remote(passed.at[c], passed_in.at[c], out_send.at[c], out_recv.at[c], col=half * (LINE - 1))

    def emit(c, hidden, squares):
        rows = pl.ds(pl.multiple_of(c * BLOCK_ROWS, BLOCK_ROWS), BLOCK_ROWS)
        scale = 1.0 / jnp.sqrt(0.25 + squares / D)
        out[rows, :] = (hidden * scale).astype(jnp.bfloat16).T

    def gather(k, b):
        used = tile_count[b]
        summed = None
        for q in range(groups):
            blocks = [arrived[k][slot_of[tile_block[b, q * GROUP + i]]] for i in range(GROUP)]
            term = jnp.dot(
                jnp.concatenate(blocks, axis=1), hits[b * groups + q], preferred_element_type=jnp.float32
            )
            summed = term if summed is None else summed + term
        mean = summed / (used * FAN_T).astype(jnp.float32)
        mixed[k, b, :piece] = arrived[k][slot_of[b]]
        mixed[k, b, piece:] = mean.astype(jnp.bfloat16)

    def product(k, blocks):
        weights = turned_w[k].reshape(2 * span, span)
        rhs = jnp.concatenate(
            [jnp.concatenate([mixed[k, c] for c in blocks], axis=1), jnp.concatenate([near[k, c] for c in blocks], axis=1)],
            axis=0,
        )
        return jnp.dot(weights, rhs, preferred_element_type=jnp.float32)

    def early(i):
        blocks = [i * PAIR + j for j in range(PAIR)]
        for c in blocks:
            near_copy(0, c).wait_recv()
        total = product(0, blocks)
        for j, c in enumerate(blocks):
            kept_theirs[c] = total[:span, j * BLOCK_ROWS : (j + 1) * BLOCK_ROWS]
            kept_mine[c] = total[span:, j * BLOCK_ROWS : (j + 1) * BLOCK_ROWS]

    def first(c):
        near_copy(1, c).wait_recv()
        total = product(1, [c])
        part[c] = (kept_theirs[c] + total[:span]).astype(jnp.bfloat16)
        part_copy(c).start()
        kept_mine[c] = kept_mine[c] + total[span:]

    def second(c):
        part_copy(c).wait_recv()
        hidden = jnp.maximum(kept_mine[c] + part_in[c].astype(jnp.float32), 0.0)
        sums[c] = jnp.sum(hidden * hidden, axis=0, keepdims=True)
        low, high = hidden[:width], hidden[width:]
        passed[c] = jnp.where(half == 0, low, high).astype(jnp.bfloat16)
        for k in range(3):
            sum_copy(c, k).start()
        out_copy(c).start()
        kept_mine[c, :width] = jnp.where(half == 0, high, low)

    def third(c):
        sum_copy(c, 0).wait_recv()
        emit(c, kept_mine[c, :width], sums[c] + sums_in[0, c])

    take(0)

    @pl.when(at_end)
    def _():
        def send_early(c, carry):
            gather(0, c)
            near_copy(0, c).start()
            return carry

        lax.fori_loop(0, dst_blocks, send_early, 0)

    pairs = dst_blocks // PAIR

    @pl.when(inside)
    def _():
        def prelude(i, carry):
            for j in range(PAIR):
                gather(0, i * PAIR + j)

            @pl.when(i >= EARLY_LAG)
            def _():
                early(i - EARLY_LAG)

            return carry

        lax.fori_loop(0, pairs, prelude, 0)

    take(1)

    @pl.when(at_end)
    def _():
        def send_late(c, carry):
            gather(1, c)
            near_copy(1, c).start()
            return carry

        lax.fori_loop(0, dst_blocks, send_late, 0)

        def receive(c, carry):
            out_copy(c).wait_recv()
            sum_copy(c, 1).wait_recv()
            sum_copy(c, 2).wait_recv()
            emit(c, passed_in[c].astype(jnp.float32), sums_in[1, c] + sums_in[2, c])
            for k in range(PARTS):
                near_copy(k, c).wait_send()
            return carry

        lax.fori_loop(0, dst_blocks, receive, 0)
        weight_copy().wait_send()

    @pl.when(inside)
    def _():
        def late(c):
            gather(1, c)

        def stage(i, carry):
            due = i - NEAR_LAG + 1

            @pl.when(jnp.logical_and(jnp.logical_and(due >= (pairs - EARLY_LAG) * PAIR, due < dst_blocks), due % PAIR == 0))
            def _():
                early(due // PAIR)

            for lag, work in ((0, late), (NEAR_LAG, first), (SWAP_LAG, second), (SUM_LAG, third)):

                @pl.when(jnp.logical_and(i >= lag, i < dst_blocks + lag))
                def _(lag=lag, work=work):
                    work(i - lag)

            return carry

        lax.fori_loop(0, dst_blocks + SUM_LAG, stage, 0)

        def finish(c, carry):
            part_copy(c).wait_send()
            for k in range(3):
                sum_copy(c, k).wait_send()
            out_copy(c).wait_send()
            return carry

        lax.fori_loop(0, dst_blocks, finish, 0)
        swap_copy(core).wait_send()

    def sent(d, carry):
        peer = lax.rem(me + d, n_dom)
        for k in range(PARTS):
            block_copy(k, peer, me).wait_send()
        return carry

    lax.fori_loop(1, n_dom, sent, 0)


def deliver_kernel(src, dst, sem):
    copy = pltpu.make_async_copy(src, dst, sem)
    copy.start()
    copy.wait()


def deliver(result):
    return pl.pallas_call(
        deliver_kernel,
        out_shape=jax.ShapeDtypeStruct(result.shape, result.dtype),
        in_specs=[pl.BlockSpec(memory_space=pltpu.VMEM)],
        out_specs=pl.BlockSpec(memory_space=pltpu.HBM),
        scratch_shapes=[pltpu.SemaphoreType.DMA],
        compiler_params=pltpu.CompilerParams(vmem_limit_bytes=8_000_000),
    )(result)


def on_line(features, requests, counts, tile_block, local_nbr, tile_count, w_self, w_neigh):
    n_dom = lax.axis_size("dom")
    total, width = local_nbr.shape[0], features.shape[1]
    dst_blocks = total // BLOCK_ROWS
    span = 2 * width
    blocks = features.reshape(-1, BLOCK_ROWS, width)
    anywhere = pl.BlockSpec(memory_space=pl.ANY)
    dma = pltpu.SemaphoreType.DMA
    bf16, f32 = jnp.bfloat16, jnp.float32
    result = pl.pallas_call(
        functools.partial(line_kernel, n_dom),
        out_shape=pltpu.VMEM((total, width), bf16),
        in_specs=[anywhere] * 8,
        out_specs=pl.BlockSpec(memory_space=pltpu.VMEM),
        scratch_shapes=[
            pltpu.VMEM(blocks.shape, bf16),
            pltpu.VMEM((PARTS, n_dom * CAP, width // PARTS, BLOCK_ROWS), bf16),
            pltpu.VMEM((n_dom * CAP, width // PARTS, BLOCK_ROWS), bf16),
            pltpu.VMEM((n_dom * CAP, width // PARTS, BLOCK_ROWS), bf16),
            pltpu.VMEM(local_nbr.shape, jnp.int32),
            pltpu.VMEM((TILES * FAN_T, BLOCK_ROWS), f32),
            pltpu.VMEM((dst_blocks * TILES // GROUP, GROUP * BLOCK_ROWS, BLOCK_ROWS), bf16),
            pltpu.VMEM((PARTS, dst_blocks, span // PARTS, BLOCK_ROWS), bf16),
            pltpu.VMEM((PARTS, dst_blocks, span // PARTS, BLOCK_ROWS), bf16),
            pltpu.VMEM((dst_blocks, span, BLOCK_ROWS), bf16),
            pltpu.VMEM((dst_blocks, span, BLOCK_ROWS), bf16),
            pltpu.VMEM((dst_blocks, span, BLOCK_ROWS), f32),
            pltpu.VMEM((dst_blocks, span, BLOCK_ROWS), f32),
            pltpu.VMEM((dst_blocks, 1, BLOCK_ROWS), f32),
            pltpu.VMEM((3, dst_blocks, 1, BLOCK_ROWS), f32),
            pltpu.VMEM((dst_blocks, width, BLOCK_ROWS), bf16),
            pltpu.VMEM((dst_blocks, width, BLOCK_ROWS), bf16),
            pltpu.VMEM((2,) + w_self.shape, bf16),
            pltpu.VMEM((2,) + w_self.shape, bf16),
            pltpu.VMEM((PARTS, 2, span, 2 * span // PARTS), bf16),
            pltpu.SMEM(requests.shape, jnp.int32),
            pltpu.SMEM(counts.shape[:1], jnp.int32),
            pltpu.SMEM(tile_block.shape, jnp.int32),
            pltpu.SMEM(tile_count.shape, jnp.int32),
            pltpu.SMEM((n_dom * CAP // 2,), jnp.int32),
            dma((8,)), dma((PARTS,)), dma((PARTS, n_dom)), dma((PARTS, n_dom)), dma, dma, dma, dma,
        ]
        + [dma((PARTS, dst_blocks))] * 2
        + [dma((dst_blocks,))] * 4
        + [dma((3, dst_blocks))] * 2,
        compiler_params=pltpu.CompilerParams(has_side_effects=True, collective_id=0, vmem_limit_bytes=56000000),
    )(requests, counts.reshape(-1), tile_block, tile_count, blocks, local_nbr, w_self, w_neigh)
    return deliver(result)


def on_device(features, requests, counts, tile_block, local_nbr, tile_count, w_self, w_neigh):
    n_dom = lax.axis_size("dom")
    n_col = lax.axis_size("col")
    col_width = features.shape[1]
    if n_col == LINE:
        return on_line(features, requests, counts, tile_block, local_nbr, tile_count, w_self, w_neigh)
    blocks = features.reshape(-1, BLOCK_ROWS, col_width)
    outgoing = blocks.at[requests[0].reshape(-1)].get(mode="promise_in_bounds")
    outgoing = outgoing.reshape(n_dom, CAP, BLOCK_ROWS, col_width)
    arrived = exchange(outgoing).reshape(n_dom * CAP, BLOCK_ROWS, col_width)
    slot_ends = jnp.cumsum(counts[:, 0])
    positions = jnp.arange(n_dom * CAP // 2, dtype=jnp.int32)
    passed = slot_ends[None, :] <= positions[:, None]
    owner_of = jnp.sum(passed.astype(jnp.int32), axis=1)
    start_of = jnp.max(jnp.where(passed, slot_ends[None, :], 0), axis=1)
    slot_of = owner_of * CAP + positions - start_of

    mixed = aggregate(arrived, slot_of, tile_block, local_nbr, tile_count)
    weights = [w_self, w_neigh]
    for shift in range(1, n_col):
        perm = [(k, (k + shift) % n_col) for k in range(n_col)]
        weights.append(lax.ppermute(w_self, "col", perm))
        weights.append(lax.ppermute(w_neigh, "col", perm))
    order = (lax.axis_index("col") - jnp.arange(n_col, dtype=jnp.int32)) % n_col
    mixed = mixed.reshape(n_col, -1, 2 * col_width)
    mixed = lax.all_to_all(mixed, "col", split_axis=0, concat_axis=0, tiled=True)
    result = project(mixed, weights, order)
    result = lax.all_to_all(result, "col", split_axis=0, concat_axis=0, tiled=True)
    return result.reshape(-1, col_width)


def solution(mesh):
    return jax.shard_map(
        on_device,
        mesh=mesh,
        in_specs=(
            P("dom", "col"),
            P("dom", None, None),
            P(None, "dom"),
            P("dom", None),
            P("dom", None),
            P("dom"),
            P("col", None),
            P("col", None),
        ),
        out_specs=P("dom", "col"),
        check_vma=False,
    )
```

```python
import functools

import jax
import jax.numpy as jnp
from jax import lax
from jax.experimental import pallas as pl
from jax.experimental.pallas import tpu as pltpu
from jax.sharding import PartitionSpec as P

D = 1024
BLOCK_ROWS = 128
CAP = 8
TILES = 32
FAN_T = 4
GROUP = 8
PACK = 16


def aggregate_kernel(
    front, width, slot_of, tile_block, tile_count, nbr_ref, arrived, out_ref, held, turned, nbr_t, sems
):
    step = pl.program_id(0)

    def fetch(p):
        return pltpu.make_async_copy(arrived.at[slot_of[p]], held.at[p], sems.at[p])

    @pl.when(step == 0)
    def _():
        def begin(p, carry):
            fetch(p).start()
            return carry

        lax.fori_loop(0, front, begin, 0)

        def finish(i, carry):
            for k in range(4):
                fetch(i * 4 + k).wait()
            for k in range(4):
                turned[i * 4 + k] = held[i * 4 + k].T
            return carry

        lax.fori_loop(0, front // 4, finish, 0)

    nbr_t[...] = nbr_ref[...].astype(jnp.float32).T
    used = tile_count[step]
    shape = (BLOCK_ROWS // PACK, PACK, BLOCK_ROWS)
    row_ids = (
        lax.broadcasted_iota(jnp.int32, shape, 0) * PACK + lax.broadcasted_iota(jnp.int32, shape, 1)
    ).astype(jnp.float32).astype(jnp.bfloat16)
    one = jnp.ones(shape, jnp.bfloat16)
    zero = jnp.zeros(shape, jnp.bfloat16)

    def body(q, acc):
        nbr = nbr_t[pl.ds(pl.multiple_of(q * (GROUP * FAN_T), GROUP * FAN_T), GROUP * FAN_T), :]
        counts = []
        blocks = []
        for i in range(GROUP):
            tile = q * GROUP + i
            total = None
            for f in range(FAN_T):
                row = nbr[i * FAN_T + f : i * FAN_T + f + 1, :]
                row = jnp.where(tile < used, row, -1.0)
                row = jnp.broadcast_to(row, (PACK, BLOCK_ROWS)).astype(jnp.bfloat16)
                hit = jnp.where(row[None] == row_ids, one, zero)
                total = hit if total is None else total + hit
            counts.append(total.reshape(BLOCK_ROWS, BLOCK_ROWS))
            blocks.append(turned[tile_block[step * TILES + tile]])
        lhs = jnp.concatenate(blocks, axis=1)
        rhs = jnp.concatenate(counts, axis=0)
        return acc + jnp.dot(lhs, rhs, preferred_element_type=jnp.float32)

    summed = lax.fori_loop(
        0, (used + GROUP - 1) // GROUP, body, jnp.zeros((width, BLOCK_ROWS), jnp.float32)
    )
    mean = summed / (used * FAN_T).astype(jnp.float32)
    out_ref[:, :width] = held[step]
    out_ref[:, width:] = mean.T.astype(jnp.bfloat16)


def aggregate(arrived, slot_of, tile_block, local_nbr, tile_count):
    front = slot_of.shape[0]
    width = arrived.shape[-1]
    dst_blocks = tile_count.shape[0]
    return pl.pallas_call(
        functools.partial(aggregate_kernel, front, width),
        out_shape=jax.ShapeDtypeStruct((dst_blocks * BLOCK_ROWS, 2 * width), jnp.bfloat16),
        grid_spec=pltpu.PrefetchScalarGridSpec(
            num_scalar_prefetch=3,
            grid=(dst_blocks,),
            in_specs=[
                pl.BlockSpec((BLOCK_ROWS, TILES * FAN_T), lambda i, *_: (i, 0)),
                pl.BlockSpec(memory_space=pl.ANY),
            ],
            out_specs=pl.BlockSpec((BLOCK_ROWS, 2 * width), lambda i, *_: (i, 0)),
            scratch_shapes=[
                pltpu.VMEM((front, BLOCK_ROWS, width), jnp.bfloat16),
                pltpu.VMEM((front, width, BLOCK_ROWS), jnp.bfloat16),
                pltpu.VMEM((TILES * FAN_T, BLOCK_ROWS), jnp.float32),
                pltpu.SemaphoreType.DMA((front,)),
            ],
        ),
        compiler_params=pltpu.CompilerParams(dimension_semantics=("arbitrary",)),
        cost_estimate=pl.CostEstimate(flops=4 * 10**9, bytes_accessed=8 * 2**20, transcendentals=0),
    )(slot_of, tile_block.reshape(-1), tile_count, local_nbr, arrived)


def project_kernel(n_col, width, order, x_ref, *rest):
    w_refs = rest[:-1]
    out_ref = rest[-1]
    total = None
    for s in range(n_col):
        rows = x_ref[order[s]]
        term = jnp.dot(rows[:, :width], w_refs[2 * s][...], preferred_element_type=jnp.float32)
        term = term + jnp.dot(rows[:, width:], w_refs[2 * s + 1][...], preferred_element_type=jnp.float32)
        total = term if total is None else total + term
    hidden = jnp.maximum(total, 0.0)
    squares = jnp.sum(hidden * hidden, axis=1, keepdims=True)
    result = (hidden / jnp.sqrt(0.25 + squares / D)).astype(jnp.bfloat16)
    for k in range(n_col):
        out_ref[k] = result[:, k * width : (k + 1) * width]


def project(mixed, weights, order):
    n_col, rows, _ = mixed.shape
    width = D // n_col
    tile = BLOCK_ROWS
    return pl.pallas_call(
        functools.partial(project_kernel, n_col, width),
        out_shape=jax.ShapeDtypeStruct((n_col, rows, width), jnp.bfloat16),
        grid_spec=pltpu.PrefetchScalarGridSpec(
            num_scalar_prefetch=1,
            grid=(rows // tile,),
            in_specs=[pl.BlockSpec((n_col, tile, 2 * width), lambda i, *_: (0, i, 0))]
            + [pl.BlockSpec((width, D), lambda i, *_: (0, 0)) for _ in weights],
            out_specs=pl.BlockSpec((n_col, tile, width), lambda i, *_: (0, i, 0)),
        ),
        compiler_params=pltpu.CompilerParams(dimension_semantics=("arbitrary",)),
        cost_estimate=pl.CostEstimate(flops=2 * 10**9, bytes_accessed=7 * 2**20, transcendentals=0),
    )(order, mixed, *weights)


MESH = pl.DeviceIdType.MESH
PARTS = 2
PAIR = 2
EARLY_LAG = 6
NEAR_LAG = 3
SWAP_LAG = 6
SUM_LAG = 9
LINE = 4
DELIVER = 2


def exchange_kernel(n_dom, outgoing, arrived, send, recv, own_sem):
    me = lax.axis_index("dom")

    def copy_to(d):
        peer = lax.rem(me + d, n_dom)
        return pltpu.make_async_remote_copy(
            src_ref=outgoing.at[peer], dst_ref=arrived.at[me], send_sem=send.at[d], recv_sem=recv.at[d],
            device_id={"dom": peer}, device_id_type=MESH,
        )

    own = pltpu.make_async_copy(outgoing.at[me], arrived.at[me], own_sem)
    for d in range(1, n_dom):
        copy_to(d).start()
    own.start()
    own.wait()
    for d in range(1, n_dom):
        copy_to(d).wait_send()
        copy_to(d).wait_recv()


def exchange(outgoing):
    n_dom = outgoing.shape[0]
    anywhere = pl.BlockSpec(memory_space=pl.ANY)
    return pl.pallas_call(
        functools.partial(exchange_kernel, n_dom),
        out_shape=jax.ShapeDtypeStruct(outgoing.shape, outgoing.dtype),
        in_specs=[anywhere],
        out_specs=anywhere,
        scratch_shapes=[
            pltpu.SemaphoreType.DMA((n_dom,)),
            pltpu.SemaphoreType.DMA((n_dom,)),
            pltpu.SemaphoreType.DMA,
        ],
        compiler_params=pltpu.CompilerParams(has_side_effects=True),
    )(outgoing)


def line_kernel(
    n_dom, requests_in, counts_in, tile_block_in, tile_count_in, features, local_nbr, w_self, w_neigh, out,
    feat, outgoing, arrived_early, arrived_late, nbr_in, nbr_t, hits, mixed, near, part, part_in, kept_theirs, kept_mine, sums, sums_in, passed, passed_in,
    own_w, far_w, turned_w, requests, counts, tile_block, tile_count, slot_of,
    load_sem, own_sem, send, recv, w_send, w_recv, swap_send, swap_recv,
    near_send, near_recv, part_send, part_recv, out_send, out_recv, sum_send, sum_recv,
):
    me = lax.axis_index("dom")
    z = lax.axis_index("col")
    core = lax.rem(me, 2)
    chip = me // 2
    n_chip = n_dom // 2
    front = slot_of.shape[0]
    _, dst_blocks, width, _ = mixed.shape
    span = 2 * width
    piece = width // PARTS
    at_end = jnp.logical_or(z == 0, z == LINE - 1)
    inside = jnp.logical_not(at_end)
    half = z // 2

    arrived = (arrived_early, arrived_late)

    def remote(src, dst, s_sem, r_sem, **device):
        return pltpu.make_async_remote_copy(
            src_ref=src, dst_ref=dst, send_sem=s_sem, recv_sem=r_sem, device_id=device, device_id_type=MESH,
        )

    barrier = pltpu.get_barrier_semaphore()

    def greet(d, carry):
        pl.semaphore_signal(barrier, inc=1, device_id={"dom": lax.rem(me + d, n_dom)}, device_id_type=MESH)
        return carry

    lax.fori_loop(1, n_dom, greet, 0)

    for inner in (1, 2):

        @pl.when(z != inner)
        def _(inner=inner):
            pl.semaphore_signal(barrier, inc=1, device_id={"col": inner}, device_id_type=MESH)

    @pl.when(inside)
    def _():
        pl.semaphore_signal(barrier, inc=1, device_id={"col": 0}, device_id_type=MESH)
        pl.semaphore_signal(barrier, inc=1, device_id={"col": LINE - 1}, device_id_type=MESH)

    loads = [
        pltpu.make_async_copy(src, dst, load_sem.at[i])
        for i, (src, dst) in enumerate(
            (
                (requests_in, requests),
                (features, feat),
                (counts_in, counts),
                (tile_count_in, tile_count),
                (tile_block_in, tile_block),
                (w_self, own_w.at[0]),
                (w_neigh, own_w.at[1]),
                (local_nbr, nbr_in),
            )
        )
    ]
    for copy in loads:
        copy.start()

    @pl.when(inside)
    def _():
        pl.semaphore_wait(barrier, n_dom + 2)

    @pl.when(at_end)
    def _():
        pl.semaphore_wait(barrier, n_dom + 1)

    def weight_copy():
        return remote(own_w.at[core], far_w.at[core], w_send, w_recv, col=1 + half)

    def swap_copy(which):
        return remote(far_w.at[which], far_w.at[which], swap_send, swap_recv, dom=me + 1 - 2 * core)

    def slots(owner):
        return pl.ds(owner * CAP, CAP)

    def block_copy(k, peer, owner):
        return remote(
            outgoing.at[k, slots(peer)], arrived[k].at[slots(owner)], send.at[k, peer], recv.at[k, owner], dom=peer
        )

    def own_copy(k):
        return pltpu.make_async_copy(outgoing.at[k, slots(me)], arrived[k].at[slots(me)], own_sem.at[k])

    loads[0].wait()
    loads[1].wait()

    def peer_of(group, turn):
        if n_chip == 4:
            column = lax.rem(chip, 2)
            toward = jnp.where(
                turn == 0, 3 - chip,
                jnp.where(turn == 1, lax.rem(chip + 2, 4), jnp.where(turn == 2, chip + 1 - 2 * column, chip)),
            )
        else:
            toward = lax.rem(chip + 1 + turn, n_chip)
        return toward * 2 + group

    def give(k, peer):
        @pl.when(peer == me)
        def _():
            own_copy(k).start()

        @pl.when(peer != me)
        def _():
            block_copy(k, peer, me).start()

    for group in range(2):

        def pick(turn, carry, group=group):
            peer = peer_of(group, turn)
            for s in range(CAP):
                block = feat[requests[0, peer, s]].T
                for k in range(PARTS):
                    outgoing[k, peer * CAP + s] = block[k * piece : (k + 1) * piece]
            give(0, peer)
            return carry

        lax.fori_loop(0, n_chip, pick, 0)
        for k in range(1, PARTS):

            def later(turn, carry, group=group, k=k):
                give(k, peer_of(group, turn))
                return carry

            lax.fori_loop(0, n_chip, later, 0)

    for copy in loads[2:]:
        copy.wait()

    @pl.when(at_end)
    def _():
        weight_copy().start()

    ends = []
    end = jnp.int32(0)
    for o in range(n_dom):
        end = end + counts[o]
        ends.append(end)

    def place(p, carry):
        owner = jnp.int32(0)
        start = jnp.int32(0)
        for o in range(n_dom):
            passed_by = ends[o] <= p
            owner = owner + jnp.where(passed_by, 1, 0)
            start = jnp.where(passed_by, ends[o], start)
        slot_of[p] = jnp.minimum(owner * CAP + p - start, n_dom * CAP - 1)
        return carry

    lax.fori_loop(0, front, place, 0)

    shape = (BLOCK_ROWS // PACK, PACK, BLOCK_ROWS)
    row_ids = (
        lax.broadcasted_iota(jnp.int32, shape, 0) * PACK + lax.broadcasted_iota(jnp.int32, shape, 1)
    ).astype(jnp.float32).astype(jnp.bfloat16)
    one = jnp.ones(shape, jnp.bfloat16)
    zero = jnp.zeros(shape, jnp.bfloat16)
    sample = lax.broadcasted_iota(jnp.int32, (TILES * FAN_T, BLOCK_ROWS), 0)
    groups = TILES // GROUP

    def prepare(b, carry):
        picked = nbr_in[pl.ds(pl.multiple_of(b * BLOCK_ROWS, BLOCK_ROWS), BLOCK_ROWS), :].astype(jnp.float32).T
        nbr_t[...] = jnp.where(sample < tile_count[b] * FAN_T, picked, -1.0)

        def build(q, inner):
            nbr = nbr_t[pl.ds(pl.multiple_of(q * (GROUP * FAN_T), GROUP * FAN_T), GROUP * FAN_T), :]
            for i in range(GROUP):
                total = None
                for f in range(FAN_T):
                    row = nbr[i * FAN_T + f : i * FAN_T + f + 1, :]
                    row = jnp.broadcast_to(row, (PACK, BLOCK_ROWS)).astype(jnp.bfloat16)
                    hit = jnp.where(row[None] == row_ids, one, zero)
                    total = hit if total is None else total + hit
                hits[b * groups + q, i * BLOCK_ROWS : (i + 1) * BLOCK_ROWS, :] = total.reshape(BLOCK_ROWS, BLOCK_ROWS)
            return inner

        return lax.fori_loop(0, groups, build, carry)

    lax.fori_loop(0, dst_blocks, prepare, 0)

    @pl.when(inside)
    def _():
        weight_copy().wait_recv()
        swap_copy(core).start()

        def turn_weights(source, base):
            for h in range(2):
                rank = jnp.where(half == h, 1, 0)
                for i in range(2):
                    turned = source[i, :, h * span : (h + 1) * span].T
                    for k in range(PARTS):
                        columns = slice(base + i * piece, base + (i + 1) * piece)
                        turned_w[k, rank, :, columns] = turned[:, k * piece : (k + 1) * piece]

        turn_weights(own_w, 0)
        swap_copy(1 - core).wait_recv()
        turn_weights(far_w, width)

    def take(k):
        own_copy(k).wait()

        def one_owner(d, carry):
            owner = lax.rem(me + d, n_dom)
            block_copy(k, owner, owner).wait_recv()
            return carry

        lax.fori_loop(1, n_dom, one_owner, 0)

    def near_copy(k, c):
        return remote(mixed.at[k, c], near.at[k, c], near_send.at[k, c], near_recv.at[k, c], col=1 + half)

    def part_copy(c):
        return remote(part.at[c], part_in.at[c], part_send.at[c], part_recv.at[c], col=2 - half)

    def sum_copy(c, k):
        target = (2 - half, half * (LINE - 1), (1 - half) * (LINE - 1))[k]
        return remote(sums.at[c], sums_in.at[k, c], sum_send.at[k, c], sum_recv.at[k, c], col=target)

    def out_copy(c):
        return remote(passed.at[c], passed_in.at[c], out_send.at[c], out_recv.at[c], col=half * (LINE - 1))

    def emit(c, hidden, squares):
        rows = pl.ds(pl.multiple_of(c * BLOCK_ROWS, BLOCK_ROWS), BLOCK_ROWS)
        scale = 1.0 / jnp.sqrt(0.25 + squares / D)
        out[rows, :] = (hidden * scale).astype(jnp.bfloat16).T

    def gather(k, b):
        used = tile_count[b]
        summed = None
        for q in range(groups):
            blocks = [arrived[k][slot_of[tile_block[b, q * GROUP + i]]] for i in range(GROUP)]
            term = jnp.dot(
                jnp.concatenate(blocks, axis=1), hits[b * groups + q], preferred_element_type=jnp.float32
            )
            summed = term if summed is None else summed + term
        mean = summed / (used * FAN_T).astype(jnp.float32)
        mixed[k, b, :piece] = arrived[k][slot_of[b]]
        mixed[k, b, piece:] = mean.astype(jnp.bfloat16)

    def product(k, blocks):
        weights = turned_w[k].reshape(2 * span, span)
        rhs = jnp.concatenate(
            [jnp.concatenate([mixed[k, c] for c in blocks], axis=1), jnp.concatenate([near[k, c] for c in blocks], axis=1)],
            axis=0,
        )
        return jnp.dot(weights, rhs, preferred_element_type=jnp.float32)

    def early(i):
        blocks = [i * PAIR + j for j in range(PAIR)]
        for c in blocks:
            near_copy(0, c).wait_recv()
        total = product(0, blocks)
        for j, c in enumerate(blocks):
            kept_theirs[c] = total[:span, j * BLOCK_ROWS : (j + 1) * BLOCK_ROWS]
            kept_mine[c] = total[span:, j * BLOCK_ROWS : (j + 1) * BLOCK_ROWS]

    def first(c):
        near_copy(1, c).wait_recv()
        rhs = jnp.concatenate([mixed[1, c], near[1, c]], axis=0)
        part[c] = (kept_theirs[c] + jnp.dot(turned_w[1, 0], rhs, preferred_element_type=jnp.float32)).astype(jnp.bfloat16)
        part_copy(c).start()
        kept_mine[c] = kept_mine[c] + jnp.dot(turned_w[1, 1], rhs, preferred_element_type=jnp.float32)

    def second(c):
        part_copy(c).wait_recv()
        hidden = jnp.maximum(kept_mine[c] + part_in[c].astype(jnp.float32), 0.0)
        sums[c] = jnp.sum(hidden * hidden, axis=0, keepdims=True)
        low, high = hidden[:width], hidden[width:]
        passed[c] = jnp.where(half == 0, low, high).astype(jnp.bfloat16)
        for k in range(3):
            sum_copy(c, k).start()
        out_copy(c).start()
        kept_mine[c, :width] = jnp.where(half == 0, high, low)

    def third(c):
        sum_copy(c, 0).wait_recv()
        emit(c, kept_mine[c, :width], sums[c] + sums_in[0, c])

    take(0)

    @pl.when(at_end)
    def _():
        def send_early(c, carry):
            gather(0, c)
            near_copy(0, c).start()
            return carry

        lax.fori_loop(0, dst_blocks, send_early, 0)

    pairs = dst_blocks // PAIR

    @pl.when(inside)
    def _():
        def prelude(i, carry):
            for j in range(PAIR):
                gather(0, i * PAIR + j)

            @pl.when(i >= EARLY_LAG)
            def _():
                early(i - EARLY_LAG)

            return carry

        lax.fori_loop(0, pairs, prelude, 0)

    take(1)

    @pl.when(at_end)
    def _():
        def send_late(c, carry):
            gather(1, c)
            near_copy(1, c).start()
            return carry

        lax.fori_loop(0, dst_blocks, send_late, 0)

        def receive(c, carry):
            out_copy(c).wait_recv()
            sum_copy(c, 1).wait_recv()
            sum_copy(c, 2).wait_recv()
            emit(c, passed_in[c].astype(jnp.float32), sums_in[1, c] + sums_in[2, c])
            for k in range(PARTS):
                near_copy(k, c).wait_send()
            return carry

        lax.fori_loop(0, dst_blocks, receive, 0)
        weight_copy().wait_send()

    @pl.when(inside)
    def _():
        def late(c):
            gather(1, c)

        def stage(i, carry):
            due = i - NEAR_LAG + 1

            @pl.when(jnp.logical_and(jnp.logical_and(due >= (pairs - EARLY_LAG) * PAIR, due < dst_blocks), due % PAIR == 0))
            def _():
                early(due // PAIR)

            for lag, work in ((0, late), (NEAR_LAG, first), (SWAP_LAG, second), (SUM_LAG, third)):

                @pl.when(jnp.logical_and(i >= lag, i < dst_blocks + lag))
                def _(lag=lag, work=work):
                    work(i - lag)

            return carry

        lax.fori_loop(0, dst_blocks + SUM_LAG, stage, 0)

        def finish(c, carry):
            part_copy(c).wait_send()
            for k in range(3):
                sum_copy(c, k).wait_send()
            out_copy(c).wait_send()
            return carry

        lax.fori_loop(0, dst_blocks, finish, 0)
        swap_copy(core).wait_send()

    def sent(d, carry):
        peer = lax.rem(me + d, n_dom)
        for k in range(PARTS):
            block_copy(k, peer, me).wait_send()
        return carry

    lax.fori_loop(1, n_dom, sent, 0)


def deliver_kernel(src, dst, sem):
    copy = pltpu.make_async_copy(src, dst, sem)
    copy.start()
    copy.wait()


def deliver(result):
    return pl.pallas_call(
        deliver_kernel,
        out_shape=jax.ShapeDtypeStruct(result.shape, result.dtype),
        in_specs=[pl.BlockSpec(memory_space=pltpu.VMEM)],
        out_specs=pl.BlockSpec(memory_space=pltpu.HBM),
        scratch_shapes=[pltpu.SemaphoreType.DMA],
        compiler_params=pltpu.CompilerParams(vmem_limit_bytes=8_000_000),
    )(result)


def on_line(features, requests, counts, tile_block, local_nbr, tile_count, w_self, w_neigh):
    n_dom = lax.axis_size("dom")
    total, width = local_nbr.shape[0], features.shape[1]
    dst_blocks = total // BLOCK_ROWS
    span = 2 * width
    blocks = features.reshape(-1, BLOCK_ROWS, width)
    anywhere = pl.BlockSpec(memory_space=pl.ANY)
    dma = pltpu.SemaphoreType.DMA
    bf16, f32 = jnp.bfloat16, jnp.float32
    result = pl.pallas_call(
        functools.partial(line_kernel, n_dom),
        out_shape=pltpu.VMEM((total, width), bf16),
        in_specs=[anywhere] * 8,
        out_specs=pl.BlockSpec(memory_space=pltpu.VMEM),
        scratch_shapes=[
            pltpu.VMEM(blocks.shape, bf16),
            pltpu.VMEM((PARTS, n_dom * CAP, width // PARTS, BLOCK_ROWS), bf16),
            pltpu.VMEM((n_dom * CAP, width // PARTS, BLOCK_ROWS), bf16),
            pltpu.VMEM((n_dom * CAP, width // PARTS, BLOCK_ROWS), bf16),
            pltpu.VMEM(local_nbr.shape, jnp.int32),
            pltpu.VMEM((TILES * FAN_T, BLOCK_ROWS), f32),
            pltpu.VMEM((dst_blocks * TILES // GROUP, GROUP * BLOCK_ROWS, BLOCK_ROWS), bf16),
            pltpu.VMEM((PARTS, dst_blocks, span // PARTS, BLOCK_ROWS), bf16),
            pltpu.VMEM((PARTS, dst_blocks, span // PARTS, BLOCK_ROWS), bf16),
            pltpu.VMEM((dst_blocks, span, BLOCK_ROWS), bf16),
            pltpu.VMEM((dst_blocks, span, BLOCK_ROWS), bf16),
            pltpu.VMEM((dst_blocks, span, BLOCK_ROWS), f32),
            pltpu.VMEM((dst_blocks, span, BLOCK_ROWS), f32),
            pltpu.VMEM((dst_blocks, 1, BLOCK_ROWS), f32),
            pltpu.VMEM((3, dst_blocks, 1, BLOCK_ROWS), f32),
            pltpu.VMEM((dst_blocks, width, BLOCK_ROWS), bf16),
            pltpu.VMEM((dst_blocks, width, BLOCK_ROWS), bf16),
            pltpu.VMEM((2,) + w_self.shape, bf16),
            pltpu.VMEM((2,) + w_self.shape, bf16),
            pltpu.VMEM((PARTS, 2, span, 2 * span // PARTS), bf16),
            pltpu.SMEM(requests.shape, jnp.int32),
            pltpu.SMEM(counts.shape[:1], jnp.int32),
            pltpu.SMEM(tile_block.shape, jnp.int32),
            pltpu.SMEM(tile_count.shape, jnp.int32),
            pltpu.SMEM((n_dom * CAP // 2,), jnp.int32),
            dma((8,)), dma((PARTS,)), dma((PARTS, n_dom)), dma((PARTS, n_dom)), dma, dma, dma, dma,
        ]
        + [dma((PARTS, dst_blocks))] * 2
        + [dma((dst_blocks,))] * 4
        + [dma((3, dst_blocks))] * 2,
        compiler_params=pltpu.CompilerParams(has_side_effects=True, collective_id=0, vmem_limit_bytes=56000000),
    )(requests, counts.reshape(-1), tile_block, tile_count, blocks, local_nbr, w_self, w_neigh)
    return deliver(result)


def on_device(features, requests, counts, tile_block, local_nbr, tile_count, w_self, w_neigh):
    n_dom = lax.axis_size("dom")
    n_col = lax.axis_size("col")
    col_width = features.shape[1]
    if n_col == LINE:
        return on_line(features, requests, counts, tile_block, local_nbr, tile_count, w_self, w_neigh)
    blocks = features.reshape(-1, BLOCK_ROWS, col_width)
    outgoing = blocks.at[requests[0].reshape(-1)].get(mode="promise_in_bounds")
    outgoing = outgoing.reshape(n_dom, CAP, BLOCK_ROWS, col_width)
    arrived = exchange(outgoing).reshape(n_dom * CAP, BLOCK_ROWS, col_width)
    slot_ends = jnp.cumsum(counts[:, 0])
    positions = jnp.arange(n_dom * CAP // 2, dtype=jnp.int32)
    passed = slot_ends[None, :] <= positions[:, None]
    owner_of = jnp.sum(passed.astype(jnp.int32), axis=1)
    start_of = jnp.max(jnp.where(passed, slot_ends[None, :], 0), axis=1)
    slot_of = owner_of * CAP + positions - start_of

    mixed = aggregate(arrived, slot_of, tile_block, local_nbr, tile_count)
    weights = [w_self, w_neigh]
    for shift in range(1, n_col):
        perm = [(k, (k + shift) % n_col) for k in range(n_col)]
        weights.append(lax.ppermute(w_self, "col", perm))
        weights.append(lax.ppermute(w_neigh, "col", perm))
    order = (lax.axis_index("col") - jnp.arange(n_col, dtype=jnp.int32)) % n_col
    mixed = mixed.reshape(n_col, -1, 2 * col_width)
    mixed = lax.all_to_all(mixed, "col", split_axis=0, concat_axis=0, tiled=True)
    result = project(mixed, weights, order)
    result = lax.all_to_all(result, "col", split_axis=0, concat_axis=0, tiled=True)
    return result.reshape(-1, col_width)


def solution(mesh):
    return jax.shard_map(
        on_device,
        mesh=mesh,
        in_specs=(
            P("dom", "col"),
            P("dom", None, None),
            P(None, "dom"),
            P("dom", None),
            P("dom", None),
            P("dom"),
            P("col", None),
            P("col", None),
        ),
        out_specs=P("dom", "col"),
        check_vma=False,
    )
```

```python
import functools

import jax
import jax.numpy as jnp
from jax import lax
from jax.experimental import pallas as pl
from jax.experimental.pallas import tpu as pltpu
from jax.sharding import PartitionSpec as P

D = 1024
BLOCK_ROWS = 128
CAP = 8
TILES = 32
FAN_T = 4
GROUP = 8
PACK = 16


def aggregate_kernel(
    front, width, slot_of, tile_block, tile_count, nbr_ref, arrived, out_ref, held, turned, nbr_t, sems
):
    step = pl.program_id(0)

    def fetch(p):
        return pltpu.make_async_copy(arrived.at[slot_of[p]], held.at[p], sems.at[p])

    @pl.when(step == 0)
    def _():
        def begin(p, carry):
            fetch(p).start()
            return carry

        lax.fori_loop(0, front, begin, 0)

        def finish(i, carry):
            for k in range(4):
                fetch(i * 4 + k).wait()
            for k in range(4):
                turned[i * 4 + k] = held[i * 4 + k].T
            return carry

        lax.fori_loop(0, front // 4, finish, 0)

    nbr_t[...] = nbr_ref[...].astype(jnp.float32).T
    used = tile_count[step]
    shape = (BLOCK_ROWS // PACK, PACK, BLOCK_ROWS)
    row_ids = (
        lax.broadcasted_iota(jnp.int32, shape, 0) * PACK + lax.broadcasted_iota(jnp.int32, shape, 1)
    ).astype(jnp.float32).astype(jnp.bfloat16)
    one = jnp.ones(shape, jnp.bfloat16)
    zero = jnp.zeros(shape, jnp.bfloat16)

    def body(q, acc):
        nbr = nbr_t[pl.ds(pl.multiple_of(q * (GROUP * FAN_T), GROUP * FAN_T), GROUP * FAN_T), :]
        counts = []
        blocks = []
        for i in range(GROUP):
            tile = q * GROUP + i
            total = None
            for f in range(FAN_T):
                row = nbr[i * FAN_T + f : i * FAN_T + f + 1, :]
                row = jnp.where(tile < used, row, -1.0)
                row = jnp.broadcast_to(row, (PACK, BLOCK_ROWS)).astype(jnp.bfloat16)
                hit = jnp.where(row[None] == row_ids, one, zero)
                total = hit if total is None else total + hit
            counts.append(total.reshape(BLOCK_ROWS, BLOCK_ROWS))
            blocks.append(turned[tile_block[step * TILES + tile]])
        lhs = jnp.concatenate(blocks, axis=1)
        rhs = jnp.concatenate(counts, axis=0)
        return acc + jnp.dot(lhs, rhs, preferred_element_type=jnp.float32)

    summed = lax.fori_loop(
        0, (used + GROUP - 1) // GROUP, body, jnp.zeros((width, BLOCK_ROWS), jnp.float32)
    )
    mean = summed / (used * FAN_T).astype(jnp.float32)
    out_ref[:, :width] = held[step]
    out_ref[:, width:] = mean.T.astype(jnp.bfloat16)


def aggregate(arrived, slot_of, tile_block, local_nbr, tile_count):
    front = slot_of.shape[0]
    width = arrived.shape[-1]
    dst_blocks = tile_count.shape[0]
    return pl.pallas_call(
        functools.partial(aggregate_kernel, front, width),
        out_shape=jax.ShapeDtypeStruct((dst_blocks * BLOCK_ROWS, 2 * width), jnp.bfloat16),
        grid_spec=pltpu.PrefetchScalarGridSpec(
            num_scalar_prefetch=3,
            grid=(dst_blocks,),
            in_specs=[
                pl.BlockSpec((BLOCK_ROWS, TILES * FAN_T), lambda i, *_: (i, 0)),
                pl.BlockSpec(memory_space=pl.ANY),
            ],
            out_specs=pl.BlockSpec((BLOCK_ROWS, 2 * width), lambda i, *_: (i, 0)),
            scratch_shapes=[
                pltpu.VMEM((front, BLOCK_ROWS, width), jnp.bfloat16),
                pltpu.VMEM((front, width, BLOCK_ROWS), jnp.bfloat16),
                pltpu.VMEM((TILES * FAN_T, BLOCK_ROWS), jnp.float32),
                pltpu.SemaphoreType.DMA((front,)),
            ],
        ),
        compiler_params=pltpu.CompilerParams(dimension_semantics=("arbitrary",)),
        cost_estimate=pl.CostEstimate(flops=4 * 10**9, bytes_accessed=8 * 2**20, transcendentals=0),
    )(slot_of, tile_block.reshape(-1), tile_count, local_nbr, arrived)


def project_kernel(n_col, width, order, x_ref, *rest):
    w_refs = rest[:-1]
    out_ref = rest[-1]
    total = None
    for s in range(n_col):
        rows = x_ref[order[s]]
        term = jnp.dot(rows[:, :width], w_refs[2 * s][...], preferred_element_type=jnp.float32)
        term = term + jnp.dot(rows[:, width:], w_refs[2 * s + 1][...], preferred_element_type=jnp.float32)
        total = term if total is None else total + term
    hidden = jnp.maximum(total, 0.0)
    squares = jnp.sum(hidden * hidden, axis=1, keepdims=True)
    result = (hidden / jnp.sqrt(0.25 + squares / D)).astype(jnp.bfloat16)
    for k in range(n_col):
        out_ref[k] = result[:, k * width : (k + 1) * width]


def project(mixed, weights, order):
    n_col, rows, _ = mixed.shape
    width = D // n_col
    tile = BLOCK_ROWS
    return pl.pallas_call(
        functools.partial(project_kernel, n_col, width),
        out_shape=jax.ShapeDtypeStruct((n_col, rows, width), jnp.bfloat16),
        grid_spec=pltpu.PrefetchScalarGridSpec(
            num_scalar_prefetch=1,
            grid=(rows // tile,),
            in_specs=[pl.BlockSpec((n_col, tile, 2 * width), lambda i, *_: (0, i, 0))]
            + [pl.BlockSpec((width, D), lambda i, *_: (0, 0)) for _ in weights],
            out_specs=pl.BlockSpec((n_col, tile, width), lambda i, *_: (0, i, 0)),
        ),
        compiler_params=pltpu.CompilerParams(dimension_semantics=("arbitrary",)),
        cost_estimate=pl.CostEstimate(flops=2 * 10**9, bytes_accessed=7 * 2**20, transcendentals=0),
    )(order, mixed, *weights)


MESH = pl.DeviceIdType.MESH
PARTS = 2
PAIR = 2
EARLY_LAG = 4
NEAR_LAG = 2
SWAP_LAG = 5
SUM_LAG = 8
LINE = 4
DELIVER = 2


def exchange_kernel(n_dom, outgoing, arrived, send, recv, own_sem):
    me = lax.axis_index("dom")

    def copy_to(d):
        peer = lax.rem(me + d, n_dom)
        return pltpu.make_async_remote_copy(
            src_ref=outgoing.at[peer], dst_ref=arrived.at[me], send_sem=send.at[d], recv_sem=recv.at[d],
            device_id={"dom": peer}, device_id_type=MESH,
        )

    own = pltpu.make_async_copy(outgoing.at[me], arrived.at[me], own_sem)
    for d in range(1, n_dom):
        copy_to(d).start()
    own.start()
    own.wait()
    for d in range(1, n_dom):
        copy_to(d).wait_send()
        copy_to(d).wait_recv()


def exchange(outgoing):
    n_dom = outgoing.shape[0]
    anywhere = pl.BlockSpec(memory_space=pl.ANY)
    return pl.pallas_call(
        functools.partial(exchange_kernel, n_dom),
        out_shape=jax.ShapeDtypeStruct(outgoing.shape, outgoing.dtype),
        in_specs=[anywhere],
        out_specs=anywhere,
        scratch_shapes=[
            pltpu.SemaphoreType.DMA((n_dom,)),
            pltpu.SemaphoreType.DMA((n_dom,)),
            pltpu.SemaphoreType.DMA,
        ],
        compiler_params=pltpu.CompilerParams(has_side_effects=True),
    )(outgoing)


def line_kernel(
    n_dom, requests_in, counts_in, tile_block_in, tile_count_in, features, local_nbr, w_self, w_neigh, out,
    feat, outgoing, arrived_early, arrived_late, nbr_in, nbr_t, hits, mixed, near, part, part_in, kept_theirs, kept_mine, sums, sums_in, passed, passed_in,
    own_w, far_w, turned_w, requests, counts, tile_block, tile_count, slot_of,
    load_sem, own_sem, send, recv, w_send, w_recv, swap_send, swap_recv,
    near_send, near_recv, part_send, part_recv, out_send, out_recv, sum_send, sum_recv,
):
    me = lax.axis_index("dom")
    z = lax.axis_index("col")
    core = lax.rem(me, 2)
    chip = me // 2
    n_chip = n_dom // 2
    front = slot_of.shape[0]
    _, dst_blocks, width, _ = mixed.shape
    span = 2 * width
    piece = width // PARTS
    at_end = jnp.logical_or(z == 0, z == LINE - 1)
    inside = jnp.logical_not(at_end)
    half = z // 2

    arrived = (arrived_early, arrived_late)

    def remote(src, dst, s_sem, r_sem, **device):
        return pltpu.make_async_remote_copy(
            src_ref=src, dst_ref=dst, send_sem=s_sem, recv_sem=r_sem, device_id=device, device_id_type=MESH,
        )

    barrier = pltpu.get_barrier_semaphore()

    def greet(d, carry):
        pl.semaphore_signal(barrier, inc=1, device_id={"dom": lax.rem(me + d, n_dom)}, device_id_type=MESH)
        return carry

    lax.fori_loop(1, n_dom, greet, 0)

    for inner in (1, 2):

        @pl.when(z != inner)
        def _(inner=inner):
            pl.semaphore_signal(barrier, inc=1, device_id={"col": inner}, device_id_type=MESH)

    @pl.when(inside)
    def _():
        pl.semaphore_signal(barrier, inc=1, device_id={"col": 0}, device_id_type=MESH)
        pl.semaphore_signal(barrier, inc=1, device_id={"col": LINE - 1}, device_id_type=MESH)

    loads = [
        pltpu.make_async_copy(src, dst, load_sem.at[i])
        for i, (src, dst) in enumerate(
            (
                (requests_in, requests),
                (features, feat),
                (counts_in, counts),
                (tile_count_in, tile_count),
                (tile_block_in, tile_block),
                (w_self, own_w.at[0]),
                (w_neigh, own_w.at[1]),
                (local_nbr, nbr_in),
            )
        )
    ]
    for copy in loads:
        copy.start()

    @pl.when(inside)
    def _():
        pl.semaphore_wait(barrier, n_dom + 2)

    @pl.when(at_end)
    def _():
        pl.semaphore_wait(barrier, n_dom + 1)

    def weight_copy():
        return remote(own_w.at[core], far_w.at[core], w_send, w_recv, col=1 + half)

    def swap_copy(which):
        return remote(far_w.at[which], far_w.at[which], swap_send, swap_recv, dom=me + 1 - 2 * core)

    def slots(owner):
        return pl.ds(owner * CAP, CAP)

    def block_copy(k, peer, owner):
        return remote(
            outgoing.at[k, slots(peer)], arrived[k].at[slots(owner)], send.at[k, peer], recv.at[k, owner], dom=peer
        )

    def own_copy(k):
        return pltpu.make_async_copy(outgoing.at[k, slots(me)], arrived[k].at[slots(me)], own_sem.at[k])

    loads[0].wait()
    loads[1].wait()

    def peer_of(group, turn):
        if n_chip == 4:
            column = lax.rem(chip, 2)
            toward = jnp.where(
                turn == 0, 3 - chip,
                jnp.where(turn == 1, lax.rem(chip + 2, 4), jnp.where(turn == 2, chip + 1 - 2 * column, chip)),
            )
        else:
            toward = lax.rem(chip + 1 + turn, n_chip)
        return toward * 2 + group

    def give(k, peer):
        @pl.when(peer == me)
        def _():
            own_copy(k).start()

        @pl.when(peer != me)
        def _():
            block_copy(k, peer, me).start()

    for group in range(2):

        def pick(turn, carry, group=group):
            peer = peer_of(group, turn)
            for s in range(CAP):
                block = feat[requests[0, peer, s]].T
                for k in range(PARTS):
                    outgoing[k, peer * CAP + s] = block[k * piece : (k + 1) * piece]
            give(0, peer)
            return carry

        lax.fori_loop(0, n_chip, pick, 0)
        for k in range(1, PARTS):

            def later(turn, carry, group=group, k=k):
                give(k, peer_of(group, turn))
                return carry

            lax.fori_loop(0, n_chip, later, 0)

    for copy in loads[2:]:
        copy.wait()

    @pl.when(at_end)
    def _():
        weight_copy().start()

    ends = []
    end = jnp.int32(0)
    for o in range(n_dom):
        end = end + counts[o]
        ends.append(end)

    def place(p, carry):
        owner = jnp.int32(0)
        start = jnp.int32(0)
        for o in range(n_dom):
            passed_by = ends[o] <= p
            owner = owner + jnp.where(passed_by, 1, 0)
            start = jnp.where(passed_by, ends[o], start)
        slot_of[p] = jnp.minimum(owner * CAP + p - start, n_dom * CAP - 1)
        return carry

    lax.fori_loop(0, front, place, 0)

    shape = (BLOCK_ROWS // PACK, PACK, BLOCK_ROWS)
    row_ids = (
        lax.broadcasted_iota(jnp.int32, shape, 0) * PACK + lax.broadcasted_iota(jnp.int32, shape, 1)
    ).astype(jnp.float32).astype(jnp.bfloat16)
    one = jnp.ones(shape, jnp.bfloat16)
    zero = jnp.zeros(shape, jnp.bfloat16)
    sample = lax.broadcasted_iota(jnp.int32, (TILES * FAN_T, BLOCK_ROWS), 0)
    groups = TILES // GROUP

    def prepare(b, carry):
        picked = nbr_in[pl.ds(pl.multiple_of(b * BLOCK_ROWS, BLOCK_ROWS), BLOCK_ROWS), :].astype(jnp.float32).T
        nbr_t[...] = jnp.where(sample < tile_count[b] * FAN_T, picked, -1.0)

        def build(q, inner):
            nbr = nbr_t[pl.ds(pl.multiple_of(q * (GROUP * FAN_T), GROUP * FAN_T), GROUP * FAN_T), :]
            for i in range(GROUP):
                total = None
                for f in range(FAN_T):
                    row = nbr[i * FAN_T + f : i * FAN_T + f + 1, :]
                    row = jnp.broadcast_to(row, (PACK, BLOCK_ROWS)).astype(jnp.bfloat16)
                    hit = jnp.where(row[None] == row_ids, one, zero)
                    total = hit if total is None else total + hit
                hits[b * groups + q, i * BLOCK_ROWS : (i + 1) * BLOCK_ROWS, :] = total.reshape(BLOCK_ROWS, BLOCK_ROWS)
            return inner

        return lax.fori_loop(0, groups, build, carry)

    lax.fori_loop(0, dst_blocks, prepare, 0)

    @pl.when(inside)
    def _():
        weight_copy().wait_recv()
        swap_copy(core).start()

        def turn_weights(source, base):
            for h in range(2):
                rank = jnp.where(half == h, 1, 0)
                for i in range(2):
                    turned = source[i, :, h * span : (h + 1) * span].T
                    for k in range(PARTS):
                        columns = slice(base + i * piece, base + (i + 1) * piece)
                        turned_w[k, rank, :, columns] = turned[:, k * piece : (k + 1) * piece]

        turn_weights(own_w, 0)
        swap_copy(1 - core).wait_recv()
        turn_weights(far_w, width)

    def take(k):
        own_copy(k).wait()

        def one_owner(d, carry):
            owner = lax.rem(me + d, n_dom)
            block_copy(k, owner, owner).wait_recv()
            return carry

        lax.fori_loop(1, n_dom, one_owner, 0)

    def near_copy(k, c):
        return remote(mixed.at[k, c], near.at[k, c], near_send.at[k, c], near_recv.at[k, c], col=1 + half)

    def part_copy(c):
        return remote(part.at[c], part_in.at[c], part_send.at[c], part_recv.at[c], col=2 - half)

    def sum_copy(c, k):
        target = (2 - half, half * (LINE - 1), (1 - half) * (LINE - 1))[k]
        return remote(sums.at[c], sums_in.at[k, c], sum_send.at[k, c], sum_recv.at[k, c], col=target)

    def out_copy(c):
        return remote(passed.at[c], passed_in.at[c], out_send.at[c], out_recv.at[c], col=half * (LINE - 1))

    def emit(c, hidden, squares):
        rows = pl.ds(pl.multiple_of(c * BLOCK_ROWS, BLOCK_ROWS), BLOCK_ROWS)
        scale = 1.0 / jnp.sqrt(0.25 + squares / D)
        out[rows, :] = (hidden * scale).astype(jnp.bfloat16).T

    def gather(k, b):
        used = tile_count[b]
        summed = None
        for q in range(groups):
            blocks = [arrived[k][slot_of[tile_block[b, q * GROUP + i]]] for i in range(GROUP)]
            term = jnp.dot(
                jnp.concatenate(blocks, axis=1), hits[b * groups + q], preferred_element_type=jnp.float32
            )
            summed = term if summed is None else summed + term
        mean = summed / (used * FAN_T).astype(jnp.float32)
        mixed[k, b, :piece] = arrived[k][slot_of[b]]
        mixed[k, b, piece:] = mean.astype(jnp.bfloat16)

    def product(k, blocks):
        weights = turned_w[k].reshape(2 * span, span)
        rhs = jnp.concatenate(
            [jnp.concatenate([mixed[k, c] for c in blocks], axis=1), jnp.concatenate([near[k, c] for c in blocks], axis=1)],
            axis=0,
        )
        return jnp.dot(weights, rhs, preferred_element_type=jnp.float32)

    def early(i):
        blocks = [i * PAIR + j for j in range(PAIR)]
        for c in blocks:
            near_copy(0, c).wait_recv()
        total = product(0, blocks)
        for j, c in enumerate(blocks):
            kept_theirs[c] = total[:span, j * BLOCK_ROWS : (j + 1) * BLOCK_ROWS]
            kept_mine[c] = total[span:, j * BLOCK_ROWS : (j + 1) * BLOCK_ROWS]

    def first(c):
        near_copy(1, c).wait_recv()
        rhs = jnp.concatenate([mixed[1, c], near[1, c]], axis=0)
        part[c] = (kept_theirs[c] + jnp.dot(turned_w[1, 0], rhs, preferred_element_type=jnp.float32)).astype(jnp.bfloat16)
        part_copy(c).start()
        kept_mine[c] = kept_mine[c] + jnp.dot(turned_w[1, 1], rhs, preferred_element_type=jnp.float32)

    def second(c):
        part_copy(c).wait_recv()
        hidden = jnp.maximum(kept_mine[c] + part_in[c].astype(jnp.float32), 0.0)
        sums[c] = jnp.sum(hidden * hidden, axis=0, keepdims=True)
        for k in (2, 1, 0):
            sum_copy(c, k).start()
        low, high = hidden[:width], hidden[width:]
        passed[c] = jnp.where(half == 0, low, high).astype(jnp.bfloat16)
        out_copy(c).start()
        kept_mine[c, :width] = jnp.where(half == 0, high, low)

    def third(c):
        sum_copy(c, 0).wait_recv()
        emit(c, kept_mine[c, :width], sums[c] + sums_in[0, c])

    take(0)

    @pl.when(at_end)
    def _():
        def send_early(c, carry):
            gather(0, c)
            near_copy(0, c).start()
            return carry

        lax.fori_loop(0, dst_blocks, send_early, 0)

    pairs = dst_blocks // PAIR

    @pl.when(inside)
    def _():
        def prelude(i, carry):
            for j in range(PAIR):
                gather(0, i * PAIR + j)

            @pl.when(i >= EARLY_LAG)
            def _():
                early(i - EARLY_LAG)

            return carry

        lax.fori_loop(0, pairs, prelude, 0)

    take(1)

    @pl.when(at_end)
    def _():
        def send_late(c, carry):
            gather(1, c)
            near_copy(1, c).start()
            return carry

        lax.fori_loop(0, dst_blocks, send_late, 0)

        def receive(c, carry):
            out_copy(c).wait_recv()
            sum_copy(c, 1).wait_recv()
            sum_copy(c, 2).wait_recv()
            emit(c, passed_in[c].astype(jnp.float32), sums_in[1, c] + sums_in[2, c])
            for k in range(PARTS):
                near_copy(k, c).wait_send()
            return carry

        lax.fori_loop(0, dst_blocks, receive, 0)
        weight_copy().wait_send()

    @pl.when(inside)
    def _():
        def late(c):
            gather(1, c)

        def stage(i, carry):
            due = i - NEAR_LAG + 1

            @pl.when(jnp.logical_and(jnp.logical_and(due >= (pairs - EARLY_LAG) * PAIR, due < dst_blocks), due % PAIR == 0))
            def _():
                early(due // PAIR)

            for lag, work in ((0, late), (NEAR_LAG, first), (SWAP_LAG, second), (SUM_LAG, third)):

                @pl.when(jnp.logical_and(i >= lag, i < dst_blocks + lag))
                def _(lag=lag, work=work):
                    work(i - lag)

            return carry

        lax.fori_loop(0, dst_blocks + SUM_LAG, stage, 0)

        def finish(c, carry):
            part_copy(c).wait_send()
            for k in range(3):
                sum_copy(c, k).wait_send()
            out_copy(c).wait_send()
            return carry

        lax.fori_loop(0, dst_blocks, finish, 0)
        swap_copy(core).wait_send()

    def sent(d, carry):
        peer = lax.rem(me + d, n_dom)
        for k in range(PARTS):
            block_copy(k, peer, me).wait_send()
        return carry

    lax.fori_loop(1, n_dom, sent, 0)


def deliver_kernel(src, dst, sem):
    copy = pltpu.make_async_copy(src, dst, sem)
    copy.start()
    copy.wait()


def deliver(result):
    return pl.pallas_call(
        deliver_kernel,
        out_shape=jax.ShapeDtypeStruct(result.shape, result.dtype),
        in_specs=[pl.BlockSpec(memory_space=pltpu.VMEM)],
        out_specs=pl.BlockSpec(memory_space=pltpu.HBM),
        scratch_shapes=[pltpu.SemaphoreType.DMA],
        compiler_params=pltpu.CompilerParams(vmem_limit_bytes=8_000_000),
    )(result)


def on_line(features, requests, counts, tile_block, local_nbr, tile_count, w_self, w_neigh):
    n_dom = lax.axis_size("dom")
    total, width = local_nbr.shape[0], features.shape[1]
    dst_blocks = total // BLOCK_ROWS
    span = 2 * width
    blocks = features.reshape(-1, BLOCK_ROWS, width)
    anywhere = pl.BlockSpec(memory_space=pl.ANY)
    dma = pltpu.SemaphoreType.DMA
    bf16, f32 = jnp.bfloat16, jnp.float32
    result = pl.pallas_call(
        functools.partial(line_kernel, n_dom),
        out_shape=pltpu.VMEM((total, width), bf16),
        in_specs=[anywhere] * 8,
        out_specs=pl.BlockSpec(memory_space=pltpu.VMEM),
        scratch_shapes=[
            pltpu.VMEM(blocks.shape, bf16),
            pltpu.VMEM((PARTS, n_dom * CAP, width // PARTS, BLOCK_ROWS), bf16),
            pltpu.VMEM((n_dom * CAP, width // PARTS, BLOCK_ROWS), bf16),
            pltpu.VMEM((n_dom * CAP, width // PARTS, BLOCK_ROWS), bf16),
            pltpu.VMEM(local_nbr.shape, jnp.int32),
            pltpu.VMEM((TILES * FAN_T, BLOCK_ROWS), f32),
            pltpu.VMEM((dst_blocks * TILES // GROUP, GROUP * BLOCK_ROWS, BLOCK_ROWS), bf16),
            pltpu.VMEM((PARTS, dst_blocks, span // PARTS, BLOCK_ROWS), bf16),
            pltpu.VMEM((PARTS, dst_blocks, span // PARTS, BLOCK_ROWS), bf16),
            pltpu.VMEM((dst_blocks, span, BLOCK_ROWS), bf16),
            pltpu.VMEM((dst_blocks, span, BLOCK_ROWS), bf16),
            pltpu.VMEM((dst_blocks, span, BLOCK_ROWS), f32),
            pltpu.VMEM((dst_blocks, span, BLOCK_ROWS), f32),
            pltpu.VMEM((dst_blocks, 1, BLOCK_ROWS), f32),
            pltpu.VMEM((3, dst_blocks, 1, BLOCK_ROWS), f32),
            pltpu.VMEM((dst_blocks, width, BLOCK_ROWS), bf16),
            pltpu.VMEM((dst_blocks, width, BLOCK_ROWS), bf16),
            pltpu.VMEM((2,) + w_self.shape, bf16),
            pltpu.VMEM((2,) + w_self.shape, bf16),
            pltpu.VMEM((PARTS, 2, span, 2 * span // PARTS), bf16),
            pltpu.SMEM(requests.shape, jnp.int32),
            pltpu.SMEM(counts.shape[:1], jnp.int32),
            pltpu.SMEM(tile_block.shape, jnp.int32),
            pltpu.SMEM(tile_count.shape, jnp.int32),
            pltpu.SMEM((n_dom * CAP // 2,), jnp.int32),
            dma((8,)), dma((PARTS,)), dma((PARTS, n_dom)), dma((PARTS, n_dom)), dma, dma, dma, dma,
        ]
        + [dma((PARTS, dst_blocks))] * 2
        + [dma((dst_blocks,))] * 4
        + [dma((3, dst_blocks))] * 2,
        compiler_params=pltpu.CompilerParams(has_side_effects=True, collective_id=0, vmem_limit_bytes=56000000),
    )(requests, counts.reshape(-1), tile_block, tile_count, blocks, local_nbr, w_self, w_neigh)
    return deliver(result)


def on_device(features, requests, counts, tile_block, local_nbr, tile_count, w_self, w_neigh):
    n_dom = lax.axis_size("dom")
    n_col = lax.axis_size("col")
    col_width = features.shape[1]
    if n_col == LINE:
        return on_line(features, requests, counts, tile_block, local_nbr, tile_count, w_self, w_neigh)
    blocks = features.reshape(-1, BLOCK_ROWS, col_width)
    outgoing = blocks.at[requests[0].reshape(-1)].get(mode="promise_in_bounds")
    outgoing = outgoing.reshape(n_dom, CAP, BLOCK_ROWS, col_width)
    arrived = exchange(outgoing).reshape(n_dom * CAP, BLOCK_ROWS, col_width)
    slot_ends = jnp.cumsum(counts[:, 0])
    positions = jnp.arange(n_dom * CAP // 2, dtype=jnp.int32)
    passed = slot_ends[None, :] <= positions[:, None]
    owner_of = jnp.sum(passed.astype(jnp.int32), axis=1)
    start_of = jnp.max(jnp.where(passed, slot_ends[None, :], 0), axis=1)
    slot_of = owner_of * CAP + positions - start_of

    mixed = aggregate(arrived, slot_of, tile_block, local_nbr, tile_count)
    weights = [w_self, w_neigh]
    for shift in range(1, n_col):
        perm = [(k, (k + shift) % n_col) for k in range(n_col)]
        weights.append(lax.ppermute(w_self, "col", perm))
        weights.append(lax.ppermute(w_neigh, "col", perm))
    order = (lax.axis_index("col") - jnp.arange(n_col, dtype=jnp.int32)) % n_col
    mixed = mixed.reshape(n_col, -1, 2 * col_width)
    mixed = lax.all_to_all(mixed, "col", split_axis=0, concat_axis=0, tiled=True)
    result = project(mixed, weights, order)
    result = lax.all_to_all(result, "col", split_axis=0, concat_axis=0, tiled=True)
    return result.reshape(-1, col_width)


def solution(mesh):
    return jax.shard_map(
        on_device,
        mesh=mesh,
        in_specs=(
            P("dom", "col"),
            P("dom", None, None),
            P(None, "dom"),
            P("dom", None),
            P("dom", None),
            P("dom"),
            P("col", None),
            P("col", None),
        ),
        out_specs=P("dom", "col"),
        check_vma=False,
    )
```
